8 devices in a mesh: rep: 1 (over z), grp: 8 (over y, x, core).
Axes of the slice: x: 2, y: 2, z: 1, core: 2. Of those that a mesh axis runs over, the one named last changes fastest.
Arguments:
- x_in: bfloat16 [512, 2048], P(('rep', 'grp'))
- seq_len: int32 [512], P(('rep', 'grp'))
- k_cache: bfloat16 [512, 512, 2, 128], P(('rep', 'grp'))
- v_cache: bfloat16 [512, 512, 2, 128], P(('rep', 'grp'))
- gamma_attn: bfloat16 [2048], replicated
- w_qkv: bfloat16 [2048, 2560], replicated
- b_qkv: bfloat16 [2560], replicated
- w_proj: bfloat16 [2048, 2048], replicated
- gamma_mlp: bfloat16 [2048], replicated
- w_in: bfloat16 [2, 11008, 2048], P(None, 'grp')
- w_out: bfloat16 [11008, 2048], P('grp')
Outputs:
- output 1: bfloat16 [512, 2048], P(('rep', 'grp'))
- output 2: bfloat16 [512, 512, 2, 128], P(('rep', 'grp'))
- output 3: bfloat16 [512, 512, 2, 128], P(('rep', 'grp'))
All inputs are finite; a program needn't handle non-finite values.
Results may differ from the reference program's by a relative error of at most 0.00822354.
Values are sent between devices in bfloat16 or wider.
A program may use at most 1 GiB of HBM per device.

```python
import jax
import jax.numpy as jnp
from jax import lax

HIDDEN = 2048
HEADS = 16
KV_HEADS = 2
HEAD = 128
FFN = 11008
LMAX = 512
BATCH = 512
ROPE_BASE = 10000
QKV_WIDTH = (HEADS + 2 * KV_HEADS) * HEAD
ROT_DIM = HEAD // 2
EPS = 1e-5


def setup_inputs(seed: int = 0, part: int = 0) -> dict:
    keys = jax.random.split(jax.random.key(seed), 10)
    gamma_attn = (1.0 + 0.3 * jax.random.normal(keys[0], (HIDDEN,), jnp.float32)).astype(jnp.bfloat16)
    w_qkv = (jax.random.normal(keys[1], (HIDDEN, QKV_WIDTH), jnp.float32) * HIDDEN ** -0.5).astype(jnp.bfloat16)
    b_qkv = (0.5 * jax.random.normal(keys[2], (QKV_WIDTH,), jnp.float32)).astype(jnp.bfloat16)
    w_proj = (jax.random.normal(keys[3], (HEADS * HEAD, HIDDEN), jnp.float32) * (HEADS * HEAD) ** -0.5).astype(jnp.bfloat16)
    gamma_mlp = (1.0 + 0.3 * jax.random.normal(keys[4], (HIDDEN,), jnp.float32)).astype(jnp.bfloat16)
    w_in = (jax.random.normal(keys[5], (2, FFN, HIDDEN), jnp.float32) * HIDDEN ** -0.5).astype(jnp.bfloat16)
    w_out = (jax.random.normal(keys[6], (FFN, HIDDEN), jnp.float32) * FFN ** -0.5).astype(jnp.bfloat16)
    x_in = jax.random.normal(jax.random.fold_in(keys[7], part), (BATCH, HIDDEN), jnp.float32).astype(jnp.bfloat16)
    seq_len = jax.random.randint(jax.random.fold_in(keys[8], part), (BATCH,), 1, LMAX, dtype=jnp.int32)
    seq_len = seq_len.at[0].set(LMAX - 1).at[BATCH - 1].set(1)
    cache_keys = jax.random.split(jax.random.fold_in(keys[9], part), 3)
    cache_shape = (BATCH, LMAX, KV_HEADS, HEAD)
    k_cache = (2.0 * jax.random.normal(cache_keys[0], cache_shape, jnp.float32)).astype(jnp.bfloat16)
    drift = jnp.cumsum(jax.random.normal(cache_keys[1], cache_shape, jnp.float32), axis=1) * LMAX ** -0.5
    v_cache = (drift + jax.random.normal(cache_keys[2], cache_shape, jnp.float32)).astype(jnp.bfloat16)
    return {'x_in': x_in, 'seq_len': seq_len, 'k_cache': k_cache, 'v_cache': v_cache,
            'gamma_attn': gamma_attn, 'w_qkv': w_qkv, 'b_qkv': b_qkv, 'w_proj': w_proj,
            'gamma_mlp': gamma_mlp, 'w_in': w_in, 'w_out': w_out}


def rms_norm(vals, gain):
    mean_sq = jnp.mean(vals * vals, axis=-1, keepdims=True)
    return (vals * lax.rsqrt(mean_sq + EPS) * gain.astype(jnp.float32)).astype(jnp.bfloat16)


def rotary(vals, positions):
    inv_freq = ROPE_BASE ** (-jnp.arange(0, ROT_DIM, 2, dtype=jnp.float32) / ROT_DIM)
    angles = positions.astype(jnp.float32)[:, None] * inv_freq[None, :]
    cosine = jnp.cos(angles)[:, None, :]
    sine = jnp.sin(angles)[:, None, :]
    pairs = vals[..., :ROT_DIM].reshape(vals.shape[:-1] + (ROT_DIM // 2, 2))
    even_part = pairs[..., 0]
    odd_part = pairs[..., 1]
    rotated = jnp.stack([even_part * cosine - odd_part * sine, odd_part * cosine + even_part * sine], axis=-1)
    return jnp.concatenate([rotated.reshape(vals.shape[:-1] + (ROT_DIM,)), vals[..., ROT_DIM:]], axis=-1)


def reference(x_in, seq_len, k_cache, v_cache, gamma_attn, w_qkv, b_qkv, w_proj, gamma_mlp, w_in, w_out):
    x_f32 = x_in.astype(jnp.float32)
    normed = rms_norm(x_f32, gamma_attn)
    qkv_proj = jnp.dot(normed, w_qkv, preferred_element_type=jnp.float32) + b_qkv.astype(jnp.float32)
    q_width = HEADS * HEAD
    kv_width = KV_HEADS * HEAD
    query_rot = rotary(qkv_proj[:, :q_width].reshape(BATCH, HEADS, HEAD), seq_len).astype(jnp.bfloat16)
    key_new = rotary(qkv_proj[:, q_width:q_width + kv_width].reshape(BATCH, KV_HEADS, HEAD), seq_len).astype(jnp.bfloat16)
    value_new = qkv_proj[:, q_width + kv_width:].reshape(BATCH, KV_HEADS, HEAD).astype(jnp.bfloat16)
    positions = jnp.arange(LMAX, dtype=jnp.int32)
    at_len = (positions[None, :] == seq_len[:, None])[:, :, None, None]
    k_out = jnp.where(at_len, key_new[:, None], k_cache)
    v_out = jnp.where(at_len, value_new[:, None], v_cache)

    def one_seq(seq_args):
        q_row, k_row, v_row, length = seq_args
        q_grouped = q_row.reshape(KV_HEADS, HEADS // KV_HEADS, HEAD).astype(jnp.float32)
        attn_scores = jnp.einsum('gqd,lgd->gql', q_grouped, k_row.astype(jnp.float32)) * HEAD ** -0.5
        attn_scores = jnp.where((positions <= length)[None, None, :], attn_scores, -jnp.inf)
        attn_probs = jax.nn.softmax(attn_scores, axis=-1).astype(jnp.bfloat16)
        context = jnp.einsum('gql,lgd->gqd', attn_probs.astype(jnp.float32), v_row.astype(jnp.float32))
        return context.reshape(HEADS * HEAD).astype(jnp.bfloat16)

    context = lax.map(one_seq, (query_rot, k_out, v_out, seq_len))
    hidden = x_f32 + jnp.dot(context, w_proj, preferred_element_type=jnp.float32)
    mlp_in = rms_norm(hidden, gamma_mlp)
    gate_up = jnp.dot(mlp_in, w_in.reshape(2 * FFN, HIDDEN).T, preferred_element_type=jnp.float32)
    swiglu = (jax.nn.silu(gate_up[:, :FFN]) * gate_up[:, FFN:]).astype(jnp.bfloat16)
    mlp_out = jnp.dot(swiglu, w_out, preferred_element_type=jnp.float32)
    layer_out = (hidden + mlp_out).astype(jnp.bfloat16)
    return (layer_out, k_out, v_out)
```

```python
import functools
import jax
import jax.numpy as jnp
import numpy as np
from jax import lax
from jax.experimental import pallas as pl
from jax.experimental.pallas import tpu as pltpu
from jax.sharding import PartitionSpec as P

HEAD = 128
ROT = 64
EPS = 1e-5
SCALE = HEAD ** -0.5


def attn_kernel(len_ref, freq_ref, x_ref, ga_ref, wq_hbm, bq_ref, wp_hbm, gm_ref, kc_hbm, vc_hbm,
                hid_ref, m_ref, ko_hbm, vo_hbm,
                kbuf, vbuf, wq, wp, n_s, lens_s, q_s, kn_s, vn_s, ctx_s, ctxb_s,
                wq_sem, wp_sem, kin_sem, vin_sem, kout_sem, vout_sem,
                *, rows, blk, heads, groups, qc):
    nblk = rows // blk
    hid = x_ref.shape[1]
    keys = kbuf.shape[1]
    nq = wq.shape[1] // qc

    def wq_copy(c):
        return pltpu.make_async_copy(wq_hbm.at[:, pl.ds(c * qc, qc)], wq.at[:, pl.ds(c * qc, qc)], wq_sem.at[c])

    def kv_in(i):
        sl = pl.ds(i * blk, blk)
        return (pltpu.make_async_copy(kc_hbm.at[sl], kbuf.at[sl], kin_sem.at[i]),
                pltpu.make_async_copy(vc_hbm.at[sl], vbuf.at[sl], vin_sem.at[i]))

    def kv_out(i):
        sl = pl.ds(i * blk, blk)
        return (pltpu.make_async_copy(kbuf.at[sl], ko_hbm.at[sl], kout_sem.at[i]),
                pltpu.make_async_copy(vbuf.at[sl], vo_hbm.at[sl], vout_sem.at[i]))

    wp_copy = pltpu.make_async_copy(wp_hbm, wp, wp_sem)

    for c in range(nq):
        wq_copy(c).start()
    for i in range(min(2, nblk)):
        for cp in kv_in(i):
            cp.start()

    for b in range(rows):
        lens_s[pl.ds(b, 1), :] = jnp.full((1, HEAD), len_ref[b].astype(jnp.float32), jnp.float32)
    x32 = x_ref[...].astype(jnp.float32)
    ms = jnp.mean(x32 * x32, axis=-1, keepdims=True)
    n_s[...] = (x32 * lax.rsqrt(ms + EPS) * ga_ref[...].astype(jnp.float32)).astype(jnp.bfloat16)
    ang = lens_s[...] * freq_ref[...]
    cos = jnp.cos(ang)
    sin = jnp.sin(ang)
    lane = lax.broadcasted_iota(jnp.int32, (rows, HEAD), 1)
    even = (lane % 2) == 0
    sin = jnp.where(even, -sin, sin)

    def rot(v):
        swapped = jnp.where(even, pltpu.roll(v, HEAD - 1, 1), pltpu.roll(v, 1, 1))
        return v * cos + swapped * sin

    nxt = min(2, nblk)
    for c in range(nq):
        wq_copy(c).wait()
        if nxt < nblk and c % 2 == 1:
            for cp in kv_in(nxt):
                cp.start()
            nxt += 1
        out = jnp.dot(n_s[...], wq[:, c * qc:(c + 1) * qc], preferred_element_type=jnp.float32)
        out = out + bq_ref[:, c * qc:(c + 1) * qc].astype(jnp.float32)
        for t in range(qc // HEAD):
            hh = c * (qc // HEAD) + t
            part = out[:, t * HEAD:(t + 1) * HEAD]
            if hh < heads:
                q_s[pl.ds(hh, rows, stride=heads), :] = rot(part)
            elif hh < heads + groups:
                kn_s[pl.ds(hh - heads, rows, stride=groups), :] = rot(part)
            else:
                vn_s[pl.ds(hh - heads - groups, rows, stride=groups), :] = part
    while nxt < nblk:
        for cp in kv_in(nxt):
            cp.start()
        nxt += 1
    wp_copy.start()

    col = lax.broadcasted_iota(jnp.int32, (heads, keys), 1)
    row = lax.broadcasted_iota(jnp.int32, (heads, keys), 0)
    own = (col % groups) == (row // (heads // groups))
    pos = jnp.where(own, col // groups, keys)
    r16 = lax.broadcasted_iota(jnp.int32, (16, HEAD), 0)
    r_pos = r16 // groups
    r_first = (r16 % groups) == 0

    def insert(buf, new_s, b, length):
        base = pl.multiple_of((length // 8) * 16, 16)
        old = buf[b, pl.ds(base, 16), :]
        new = jnp.where(r_first, new_s[pl.ds(2 * b, 1), :], new_s[pl.ds(2 * b + 1, 1), :])
        buf[b, pl.ds(base, 16), :] = jnp.where(r_pos == length % 8, new, old.astype(jnp.float32)).astype(jnp.bfloat16)

    def block(i, carry):
        for cp in kv_in(i):
            cp.wait()
        for j in range(blk):
            b = i * blk + j
            length = len_ref[b]
            insert(kbuf, kn_s, b, length)
            insert(vbuf, vn_s, b, length)
        for j in range(blk):
            b = i * blk + j
            length = len_ref[b]
            q = q_s[pl.ds(b * heads, heads), :].astype(jnp.bfloat16)
            s = lax.dot_general(q, kbuf[b], (((1,), (1,)), ((), ())), preferred_element_type=jnp.float32)
            s = jnp.where(pos <= length, s * SCALE, -jnp.inf)
            p = jnp.exp(s - jnp.max(s, axis=-1, keepdims=True))
            p = p / jnp.sum(p, axis=-1, keepdims=True)
            ctx_s[pl.ds(b * heads, heads), :] = jnp.dot(p.astype(jnp.bfloat16), vbuf[b],
                                                        preferred_element_type=jnp.float32)
        for cp in kv_out(i):
            cp.start()
        return carry

    lax.fori_loop(0, nblk, block, 0)

    for h in range(heads):
        ctxb_s[:, h * HEAD:(h + 1) * HEAD] = ctx_s[pl.ds(h, rows, stride=heads), :].astype(jnp.bfloat16)
    wp_copy.wait()
    pc = 512
    for c in range(hid // pc):
        sl = slice(c * pc, (c + 1) * pc)
        hid_ref[:, sl] = x_ref[:, sl].astype(jnp.float32) + jnp.dot(
            ctxb_s[...], wp[:, sl], preferred_element_type=jnp.float32)
    h32 = hid_ref[...]
    ms = jnp.mean(h32 * h32, axis=-1, keepdims=True)
    m_ref[...] = (h32 * lax.rsqrt(ms + EPS) * gm_ref[...].astype(jnp.float32)).astype(jnp.bfloat16)

    def drain(i, carry):
        for cp in kv_out(i):
            cp.wait()
        return carry

    lax.fori_loop(0, nblk, drain, 0)


def attention(x, lens, kc, vc, ga, wqkv, bqkv, wproj, gm):
    rows, hid = x.shape
    cache_len, groups = kc.shape[1], kc.shape[2]
    heads = wproj.shape[0] // HEAD
    blk, qc = 8, 256
    nblk = rows // blk
    freq = np.zeros((1, HEAD), np.float32)
    freq[0, :ROT] = np.repeat(np.float32(10000.0) ** (-np.arange(0, ROT, 2, dtype=np.float32) / np.float32(ROT)), 2)
    keys = cache_len * groups
    kflat = kc.reshape(rows, keys, HEAD)
    vflat = vc.reshape(rows, keys, HEAD)
    vm = pl.BlockSpec(memory_space=pltpu.VMEM)
    hbm = pl.BlockSpec(memory_space=pl.ANY)
    sm = pl.BlockSpec(memory_space=pltpu.SMEM)
    bf, f32 = jnp.bfloat16, jnp.float32
    hidden, m, ko, vo = pl.pallas_call(
        functools.partial(attn_kernel, rows=rows, blk=blk, heads=heads, groups=groups, qc=qc),
        name="attn",
        out_shape=(jax.ShapeDtypeStruct((rows, hid), f32), jax.ShapeDtypeStruct((rows, hid), bf),
                   jax.ShapeDtypeStruct(kflat.shape, bf), jax.ShapeDtypeStruct(vflat.shape, bf)),
        in_specs=[sm, vm, vm, vm, hbm, vm, hbm, vm, hbm, hbm],
        out_specs=(vm, vm, hbm, hbm),
        scratch_shapes=[
            pltpu.VMEM((rows, keys, HEAD), bf), pltpu.VMEM((rows, keys, HEAD), bf),
            pltpu.VMEM(wqkv.shape, bf), pltpu.VMEM(wproj.shape, bf),
            pltpu.VMEM((rows, hid), bf), pltpu.VMEM((rows, HEAD), f32),
            pltpu.VMEM((rows * heads, HEAD), f32),
            pltpu.VMEM((rows * groups, HEAD), f32), pltpu.VMEM((rows * groups, HEAD), f32),
            pltpu.VMEM((rows * heads, HEAD), f32), pltpu.VMEM((rows, heads * HEAD), bf),
            pltpu.SemaphoreType.DMA((wqkv.shape[1] // qc,)), pltpu.SemaphoreType.DMA(()),
            pltpu.SemaphoreType.DMA((nblk,)), pltpu.SemaphoreType.DMA((nblk,)),
            pltpu.SemaphoreType.DMA((nblk,)), pltpu.SemaphoreType.DMA((nblk,)),
        ],
        compiler_params=pltpu.CompilerParams(vmem_limit_bytes=60 * 1024 * 1024),
        cost_estimate=pl.CostEstimate(flops=2 * rows * hid * 4608 + 4 * rows * heads * keys * HEAD,
                                      bytes_accessed=86000000, transcendentals=rows * heads * keys),
    )(lens, jnp.asarray(freq), x, ga.reshape(1, -1), wqkv, bqkv.reshape(1, -1), wproj, gm.reshape(1, -1), kflat, vflat)
    return hidden, m, ko.reshape(kc.shape), vo.reshape(vc.shape)


def solution(mesh):
    row_spec = P(('rep', 'grp'))
    repl_spec = P()

    def local_layer(x_in, seq_len, k_cache, v_cache, gamma_attn, w_qkv, b_qkv, w_proj, gamma_mlp, w_in, w_out):
        hidden, mlp_in, k_out, v_out = attention(x_in, seq_len, k_cache, v_cache, gamma_attn, w_qkv, b_qkv, w_proj, gamma_mlp)
        group_rows = lax.all_gather(mlp_in, 'grp', axis=0, tiled=True)
        gate_up = jnp.einsum('bh,cfh->bcf', group_rows, w_in, preferred_element_type=jnp.float32)
        swiglu = (jax.nn.silu(gate_up[:, 0]) * gate_up[:, 1]).astype(jnp.bfloat16)
        part_sum = jnp.dot(swiglu, w_out, preferred_element_type=jnp.float32).astype(jnp.bfloat16)
        mlp_out = lax.psum_scatter(part_sum, 'grp', scatter_dimension=0, tiled=True)
        layer_out = (hidden + mlp_out.astype(jnp.float32)).astype(jnp.bfloat16)
        return layer_out, k_out, v_out

    return jax.shard_map(local_layer, mesh=mesh,
                         in_specs=(row_spec, row_spec, row_spec, row_spec, repl_spec, repl_spec, repl_spec,
                                   repl_spec, repl_spec, P(None, 'grp', None), P('grp', None)),
                         out_specs=(row_spec, row_spec, row_spec), check_vma=False)
```

```python
import functools
import jax
import jax.numpy as jnp
import numpy as np
from jax import lax
from jax.experimental import pallas as pl
from jax.experimental.pallas import tpu as pltpu
from jax.sharding import PartitionSpec as P

HEAD = 128
ROT = 64
EPS = 1e-5
SCALE = HEAD ** -0.5


def attn_kernel(len_ref, freq_ref, x_ref, ga_ref, wq_hbm, bq_ref, wp_hbm, gm_ref, kc_hbm, vc_hbm,
                hid_ref, m_ref, ko_hbm, vo_hbm,
                kbuf, vbuf, wq, wp, n_s, lens_s, q_s, kn_s, vn_s, ctx_s, ctxb_s,
                wq_sem, wp_sem, kin_sem, vin_sem, kout_sem, vout_sem,
                *, rows, blk, heads, groups, qc):
    nblk = rows // blk
    hid = x_ref.shape[1]
    keys = kbuf.shape[1]
    nq = wq.shape[1] // qc

    def wq_copy(c):
        return pltpu.make_async_copy(wq_hbm.at[:, pl.ds(c * qc, qc)], wq.at[:, pl.ds(c * qc, qc)], wq_sem.at[c])

    def kv_in(i):
        sl = pl.ds(i * blk, blk)
        return (pltpu.make_async_copy(kc_hbm.at[sl], kbuf.at[sl], kin_sem.at[i]),
                pltpu.make_async_copy(vc_hbm.at[sl], vbuf.at[sl], vin_sem.at[i]))

    def kv_out(i):
        sl = pl.ds(i * blk, blk)
        return (pltpu.make_async_copy(kbuf.at[sl], ko_hbm.at[sl], kout_sem.at[i]),
                pltpu.make_async_copy(vbuf.at[sl], vo_hbm.at[sl], vout_sem.at[i]))

    wp_copy = pltpu.make_async_copy(wp_hbm, wp, wp_sem)

    for c in range(nq):
        wq_copy(c).start()
    for i in range(min(2, nblk)):
        for cp in kv_in(i):
            cp.start()

    for b in range(rows):
        lens_s[pl.ds(b, 1), :] = jnp.full((1, HEAD), len_ref[b].astype(jnp.float32), jnp.float32)
    x32 = x_ref[...].astype(jnp.float32)
    ms = jnp.mean(x32 * x32, axis=-1, keepdims=True)
    n_s[...] = (x32 * lax.rsqrt(ms + EPS) * ga_ref[...].astype(jnp.float32)).astype(jnp.bfloat16)
    ang = lens_s[...] * freq_ref[...]
    cos = jnp.cos(ang)
    sin = jnp.sin(ang)
    lane = lax.broadcasted_iota(jnp.int32, (rows, HEAD), 1)
    even = (lane % 2) == 0
    sin = jnp.where(even, -sin, sin)

    def rot(v):
        swapped = jnp.where(even, pltpu.roll(v, HEAD - 1, 1), pltpu.roll(v, 1, 1))
        return v * cos + swapped * sin

    nxt = min(2, nblk)
    for c in range(nq):
        wq_copy(c).wait()
        if nxt < nblk and c % 2 == 1:
            for cp in kv_in(nxt):
                cp.start()
            nxt += 1
        out = jnp.dot(n_s[...], wq[:, c * qc:(c + 1) * qc], preferred_element_type=jnp.float32)
        out = out + bq_ref[:, c * qc:(c + 1) * qc].astype(jnp.float32)
        for t in range(qc // HEAD):
            hh = c * (qc // HEAD) + t
            part = out[:, t * HEAD:(t + 1) * HEAD]
            if hh < heads:
                q_s[pl.ds(hh, rows, stride=heads), :] = rot(part)
            elif hh < heads + groups:
                kn_s[pl.ds(hh - heads, rows, stride=groups), :] = rot(part)
            else:
                vn_s[pl.ds(hh - heads - groups, rows, stride=groups), :] = part
    while nxt < nblk:
        for cp in kv_in(nxt):
            cp.start()
        nxt += 1
    wp_copy.start()

    col = lax.broadcasted_iota(jnp.int32, (heads, keys), 1)
    row = lax.broadcasted_iota(jnp.int32, (heads, keys), 0)
    own = (col % groups) == (row // (heads // groups))
    pos = jnp.where(own, col // groups, keys)
    r16 = lax.broadcasted_iota(jnp.int32, (16, HEAD), 0)
    r_pos = r16 // groups
    r_first = (r16 % groups) == 0

    def insert(buf, new_s, b, length):
        base = pl.multiple_of((length // 8) * 16, 16)
        old = buf[b, pl.ds(base, 16), :]
        new = jnp.where(r_first, new_s[pl.ds(2 * b, 1), :], new_s[pl.ds(2 * b + 1, 1), :])
        buf[b, pl.ds(base, 16), :] = jnp.where(r_pos == length % 8, new, old.astype(jnp.float32)).astype(jnp.bfloat16)

    def block(i, carry):
        for cp in kv_in(i):
            cp.wait()
        for j in range(blk):
            b = i * blk + j
            length = len_ref[b]
            insert(kbuf, kn_s, b, length)
            insert(vbuf, vn_s, b, length)
        for j in range(blk):
            b = i * blk + j
            length = len_ref[b]
            q = q_s[pl.ds(b * heads, heads), :].astype(jnp.bfloat16)
            s = lax.dot_general(q, kbuf[b], (((1,), (1,)), ((), ())), preferred_element_type=jnp.float32)
            s = jnp.where(pos <= length, s * SCALE, -jnp.inf)
            p = jnp.exp(s - jnp.max(s, axis=-1, keepdims=True))
            p = p / jnp.sum(p, axis=-1, keepdims=True)
            ctx_s[pl.ds(b * heads, heads), :] = jnp.dot(p.astype(jnp.bfloat16), vbuf[b],
                                                        preferred_element_type=jnp.float32)
        for cp in kv_out(i):
            cp.start()
        return carry

    lax.fori_loop(0, nblk, block, 0)

    for h in range(heads):
        ctxb_s[:, h * HEAD:(h + 1) * HEAD] = ctx_s[pl.ds(h, rows, stride=heads), :].astype(jnp.bfloat16)
    wp_copy.wait()
    pc = 512
    for c in range(hid // pc):
        sl = slice(c * pc, (c + 1) * pc)
        hid_ref[:, sl] = x_ref[:, sl].astype(jnp.float32) + jnp.dot(
            ctxb_s[...], wp[:, sl], preferred_element_type=jnp.float32)
    h32 = hid_ref[...]
    ms = jnp.mean(h32 * h32, axis=-1, keepdims=True)
    m_ref[...] = (h32 * lax.rsqrt(ms + EPS) * gm_ref[...].astype(jnp.float32)).astype(jnp.bfloat16)

    def drain(i, carry):
        for cp in kv_out(i):
            cp.wait()
        return carry

    lax.fori_loop(0, nblk, drain, 0)


def attention(x, lens, kc, vc, ga, wqkv, bqkv, wproj, gm):
    rows, hid = x.shape
    cache_len, groups = kc.shape[1], kc.shape[2]
    heads = wproj.shape[0] // HEAD
    blk, qc = 8, 256
    nblk = rows // blk
    freq = np.zeros((1, HEAD), np.float32)
    freq[0, :ROT] = np.repeat(np.float32(10000.0) ** (-np.arange(0, ROT, 2, dtype=np.float32) / np.float32(ROT)), 2)
    keys = cache_len * groups
    kflat = kc.reshape(rows, keys, HEAD)
    vflat = vc.reshape(rows, keys, HEAD)
    vm = pl.BlockSpec(memory_space=pltpu.VMEM)
    hbm = pl.BlockSpec(memory_space=pl.ANY)
    sm = pl.BlockSpec(memory_space=pltpu.SMEM)
    bf, f32 = jnp.bfloat16, jnp.float32
    hidden, m, ko, vo = pl.pallas_call(
        functools.partial(attn_kernel, rows=rows, blk=blk, heads=heads, groups=groups, qc=qc),
        name="attn",
        out_shape=(jax.ShapeDtypeStruct((rows, hid), f32), jax.ShapeDtypeStruct((rows, hid), bf),
                   jax.ShapeDtypeStruct(kflat.shape, bf), jax.ShapeDtypeStruct(vflat.shape, bf)),
        in_specs=[sm, vm, vm, vm, hbm, vm, hbm, vm, hbm, hbm],
        out_specs=(vm, vm, hbm, hbm),
        scratch_shapes=[
            pltpu.VMEM((rows, keys, HEAD), bf), pltpu.VMEM((rows, keys, HEAD), bf),
            pltpu.VMEM(wqkv.shape, bf), pltpu.VMEM(wproj.shape, bf),
            pltpu.VMEM((rows, hid), bf), pltpu.VMEM((rows, HEAD), f32),
            pltpu.VMEM((rows * heads, HEAD), f32),
            pltpu.VMEM((rows * groups, HEAD), f32), pltpu.VMEM((rows * groups, HEAD), f32),
            pltpu.VMEM((rows * heads, HEAD), f32), pltpu.VMEM((rows, heads * HEAD), bf),
            pltpu.SemaphoreType.DMA((wqkv.shape[1] // qc,)), pltpu.SemaphoreType.DMA(()),
            pltpu.SemaphoreType.DMA((nblk,)), pltpu.SemaphoreType.DMA((nblk,)),
            pltpu.SemaphoreType.DMA((nblk,)), pltpu.SemaphoreType.DMA((nblk,)),
        ],
        compiler_params=pltpu.CompilerParams(vmem_limit_bytes=60 * 1024 * 1024),
        cost_estimate=pl.CostEstimate(flops=2 * rows * hid * 4608 + 4 * rows * heads * keys * HEAD,
                                      bytes_accessed=86000000, transcendentals=rows * heads * keys),
    )(lens, jnp.asarray(freq), x, ga.reshape(1, -1), wqkv, bqkv.reshape(1, -1), wproj, gm.reshape(1, -1), kflat, vflat)
    return hidden, m, ko.reshape(kc.shape), vo.reshape(vc.shape)


def mlp_kernel(hid_ref, m_ref, wi_hbm, wo_hbm, out_ref,
               wi, wt, wo, gath, act, own_s, ps, rb, sb, rr,
               wi_sem, wt_sem, wo_sem, ag_send, ag_recv, fw_send, ps_send, ps_recv, rs_send, rs_recv,
               *, chunks, crows, full, tail, fc, nc):
    hid = m_ref.shape[1]
    ncol = hid // nc
    me = lax.axis_index('grp')
    core, xx, yy = me % 2, (me // 2) % 2, me // 4
    peer = me + 1 - 2 * core
    near_x = me + 2 - 4 * xx
    near_y = me + 4 - 8 * yy
    diag = me + 2 - 4 * xx + 4 - 8 * yy
    remote = (near_x, near_y, diag)

    def wi_copy(f, g):
        sl = pl.ds(f * fc, fc)
        return pltpu.make_async_copy(wi_hbm.at[g, sl], wi.at[g, sl], wi_sem.at[f, g])

    def wt_copy(g):
        return pltpu.make_async_copy(wi_hbm.at[g, pl.ds(full * fc, tail)], wt.at[pl.ds(g * (fc // 2), tail)], wt_sem.at[g])

    def wo_copy(c):
        return pltpu.make_async_copy(wo_hbm.at[:, pl.ds(c * nc, nc)],
                                     wo.at[pl.ds(0, full * fc + tail), pl.ds(c * nc, nc)], wo_sem.at[c])

    for f in range(full):
        for g in range(2):
            wi_copy(f, g).start()
    for g in range(2):
        wt_copy(g).start()
    for c in range(ncol):
        wo_copy(c).start()

    def rcopy(src, dst, ss, rs, dev):
        return pltpu.make_async_remote_copy(src_ref=src, dst_ref=dst, send_sem=ss, recv_sem=rs,
                                            device_id={'grp': dev}, device_id_type=pl.DeviceIdType.MESH)

    def own_send(h, q):
        slot, dev = ((4, peer), (1, near_x), (2, near_y), (3, diag))[q]
        return rcopy(m_ref.at[pl.ds(h * crows, crows)], gath.at[h, pl.ds(slot * crows, crows)],
                     ag_send.at[h, q], ag_recv.at[h, slot], dev)

    def forward(h, q):
        return rcopy(gath.at[h, pl.ds(q * crows, crows)], gath.at[h, pl.ds((q + 4) * crows, crows)],
                     fw_send.at[h, q], ag_recv.at[h, q + 4], peer)

    def pair_send(h, c):
        sl = (h, slice(None), pl.ds(c * nc, nc))
        return rcopy(ps.at[sl], rb.at[sl], ps_send.at[h, c], ps_recv.at[h, c], peer)

    def part_send(h, c, q):
        sl = (h, q, slice(None), pl.ds(c * nc, nc))
        return rcopy(sb.at[sl], rr.at[sl], rs_send.at[h, c, q], rs_recv.at[h, c, q], remote[q])

    barrier = pltpu.get_barrier_semaphore()
    for dev in (peer,) + remote:
        pl.semaphore_signal(barrier, inc=1, device_id={'grp': dev}, device_id_type=pl.DeviceIdType.MESH)
    pl.semaphore_wait(barrier, 4)

    for h in range(chunks):
        for q in (1, 2, 3, 0):
            own_send(h, q).start()

    pad = fc // 2 - tail
    for g in range(2):
        wt[g * (fc // 2) + tail:(g + 1) * (fc // 2), :] = jnp.zeros((pad, hid), jnp.bfloat16)
    wo[full * fc + tail:, :] = jnp.zeros((pad, hid), jnp.bfloat16)
    for h in range(chunks):
        gath[h, 0:crows] = m_ref[h * crows:(h + 1) * crows, :]

    nt = (((1,), (1,)), ((), ()))

    def pair_sum(h, c):
        pair_send(h, c).wait_recv()
        cs = slice(c * nc, (c + 1) * nc)
        tot = own_s[h, :, cs] + rb[h, :, cs].astype(jnp.float32)
        own_s[h, 0:crows, cs] = tot[0:crows]
        for q in range(3):
            sb[h, q, :, cs] = tot[(q + 1) * crows:(q + 2) * crows].astype(jnp.bfloat16)
        for q in (2, 0, 1):
            part_send(h, c, q).start()

    for h in range(chunks):
        for q in (1, 2, 3):
            own_send(h, q).wait_recv()
            forward(h, q).start()
        own_send(h, 0).wait_recv()
        for q in (1, 2, 3):
            forward(h, q).wait_recv()

        def in_proj(f, carry):
            if h == 0:
                for g in range(2):
                    wi_copy(f, g).wait()
            sl = pl.ds(pl.multiple_of(f * fc, fc), fc)
            gate = lax.dot_general(gath[h], wi[0, sl, :], nt, preferred_element_type=jnp.float32)
            up = lax.dot_general(gath[h], wi[1, sl, :], nt, preferred_element_type=jnp.float32)
            act[:, sl] = (jax.nn.silu(gate) * up).astype(jnp.bfloat16)
            return carry

        lax.fori_loop(0, full, in_proj, 0)
        if h == 0:
            for g in range(2):
                wt_copy(g).wait()
        gu = lax.dot_general(gath[h], wt[...], nt, preferred_element_type=jnp.float32)
        act[:, full * fc:] = (jax.nn.silu(gu[:, :fc // 2]) * gu[:, fc // 2:]).astype(jnp.bfloat16)

        half = 4 * crows
        for c in range(ncol):
            if h == 0:
                wo_copy(c).wait()
            cs = slice(c * nc, (c + 1) * nc)
            part = jnp.dot(act[...], wo[:, cs], preferred_element_type=jnp.float32)
            ps[h, :, cs] = part[half:].astype(jnp.bfloat16)
            own_s[h, :, cs] = part[:half]
            pair_send(h, c).start()
            if c > 0:
                pair_sum(h, c - 1)
        pair_sum(h, ncol - 1)

    for h in range(chunks):
        rs = slice(h * crows, (h + 1) * crows)
        for c in range(ncol):
            cs = slice(c * nc, (c + 1) * nc)
            for q in range(3):
                part_send(h, c, q).wait_recv()
            tot = hid_ref[rs, cs] + own_s[h, 0:crows, cs]
            for q in range(3):
                tot = tot + rr[h, q, :, cs].astype(jnp.float32)
            out_ref[rs, cs] = tot.astype(jnp.bfloat16)

    for h in range(chunks):
        for q in range(4):
            own_send(h, q).wait_send()
        for q in (1, 2, 3):
            forward(h, q).wait_send()
        for c in range(ncol):
            pair_send(h, c).wait_send()
            for q in range(3):
                part_send(h, c, q).wait_send()


def mlp(hidden, m, w_in, w_out):
    rows, hid = m.shape
    ffn = w_out.shape[0]
    chunks, fc, nc = 2, 256, 512
    crows = rows // chunks
    full, tail = ffn // fc, ffn % fc
    ncol = hid // nc
    vm = pl.BlockSpec(memory_space=pltpu.VMEM)
    hbm = pl.BlockSpec(memory_space=pl.ANY)
    bf, f32 = jnp.bfloat16, jnp.float32
    dma = pltpu.SemaphoreType.DMA
    return pl.pallas_call(
        functools.partial(mlp_kernel, chunks=chunks, crows=crows, full=full, tail=tail, fc=fc, nc=nc),
        name="mlp",
        out_shape=jax.ShapeDtypeStruct((rows, hid), bf),
        in_specs=[vm, vm, hbm, hbm],
        out_specs=vm,
        scratch_shapes=[
            pltpu.VMEM((2, full * fc, hid), bf), pltpu.VMEM((fc, hid), bf), pltpu.VMEM((full * fc + fc // 2, hid), bf),
            pltpu.VMEM((chunks, 8 * crows, hid), bf), pltpu.VMEM((8 * crows, full * fc + fc // 2), bf),
            pltpu.VMEM((chunks, 4 * crows, hid), f32), pltpu.VMEM((chunks, 4 * crows, hid), bf),
            pltpu.VMEM((chunks, 4 * crows, hid), bf),
            pltpu.VMEM((chunks, 3, crows, hid), bf), pltpu.VMEM((chunks, 3, crows, hid), bf),
            dma((full, 2)), dma((2,)), dma((ncol,)),
            dma((chunks, 4)), dma((chunks, 8)), dma((chunks, 4)),
            dma((chunks, ncol)), dma((chunks, ncol)), dma((chunks, ncol, 3)), dma((chunks, ncol, 3)),
        ],
        compiler_params=pltpu.CompilerParams(collective_id=0, has_side_effects=True, vmem_limit_bytes=60 * 1024 * 1024),
        cost_estimate=pl.CostEstimate(flops=2 * 8 * rows * hid * ffn * 3, bytes_accessed=17000000, transcendentals=8 * rows * ffn),
    )(hidden, m, w_in, w_out)


def solution(mesh):
    row_spec = P(('rep', 'grp'))
    repl_spec = P()

    def local_layer(x_in, seq_len, k_cache, v_cache, gamma_attn, w_qkv, b_qkv, w_proj, gamma_mlp, w_in, w_out):
        hidden, mlp_in, k_out, v_out = attention(x_in, seq_len, k_cache, v_cache, gamma_attn, w_qkv, b_qkv, w_proj, gamma_mlp)
        layer_out = mlp(hidden, mlp_in, w_in, w_out)
        return layer_out, k_out, v_out

    return jax.shard_map(local_layer, mesh=mesh,
                         in_specs=(row_spec, row_spec, row_spec, row_spec, repl_spec, repl_spec, repl_spec,
                                   repl_spec, repl_spec, P(None, 'grp', None), P('grp', None)),
                         out_specs=(row_spec, row_spec, row_spec), check_vma=False)
```

```python
import functools
import jax
import jax.numpy as jnp
import numpy as np
from jax import lax
from jax.experimental import pallas as pl
from jax.experimental.pallas import tpu as pltpu
from jax.sharding import PartitionSpec as P

HEAD = 128
ROT = 64
EPS = 1e-5
SCALE = HEAD ** -0.5
WQ_AHEAD = 10
KV_AHEAD = 4


def attn_kernel(len_hbm, freq_hbm, x_hbm, ga_hbm, wq_hbm, bq_hbm, wp_hbm, gm_hbm, kc_hbm, vc_hbm,
                hid_ref, m_ref, ko_hbm, vo_hbm,
                kbuf, vbuf, wq, wp, len_ref, freq_ref, x_ref, ga_ref, bq_ref, gm_ref,
                n_s, lens_s, q_s, kn_s, vn_s, s_s, p_s, ctx_s, ctxb_s,
                small_sem, wq_sem, wp_sem, kin_sem, vin_sem, kout_sem, vout_sem,
                *, rows, blk, heads, groups, qc):
    nblk = rows // blk
    hid = x_ref.shape[1]
    keys = kbuf.shape[1]
    nq = wq.shape[1] // qc

    small = [pltpu.make_async_copy(src, dst, small_sem.at[i]) for i, (src, dst) in enumerate((
        (x_hbm, x_ref), (len_hbm, len_ref), (ga_hbm, ga_ref), (freq_hbm, freq_ref),
        (bq_hbm, bq_ref), (gm_hbm, gm_ref)))]

    def wq_copy(c):
        return pltpu.make_async_copy(wq_hbm.at[:, pl.ds(c * qc, qc)], wq.at[:, pl.ds(c * qc, qc)], wq_sem.at[c])

    def kv_in(i):
        sl = pl.ds(i * blk, blk)
        return (pltpu.make_async_copy(kc_hbm.at[sl], kbuf.at[sl], kin_sem.at[i]),
                pltpu.make_async_copy(vc_hbm.at[sl], vbuf.at[sl], vin_sem.at[i]))

    def kv_out(i):
        sl = pl.ds(i * blk, blk)
        return (pltpu.make_async_copy(kbuf.at[sl], ko_hbm.at[sl], kout_sem.at[i]),
                pltpu.make_async_copy(vbuf.at[sl], vo_hbm.at[sl], vout_sem.at[i]))

    wp_copy = pltpu.make_async_copy(wp_hbm, wp, wp_sem)

    for cp in small:
        cp.start()
    for c in range(min(WQ_AHEAD, nq)):
        wq_copy(c).start()
    for i in range(min(KV_AHEAD, nblk)):
        for cp in kv_in(i):
            cp.start()
    for cp in small:
        cp.wait()

    for b in range(rows):
        lens_s[pl.ds(b, 1), :] = jnp.full((1, HEAD), len_ref[b].astype(jnp.float32), jnp.float32)
    x32 = x_ref[...].astype(jnp.float32)
    ms = jnp.mean(x32 * x32, axis=-1, keepdims=True)
    n_s[...] = (x32 * lax.rsqrt(ms + EPS) * ga_ref[...].astype(jnp.float32).reshape(1, hid)).astype(jnp.bfloat16)
    ang = lens_s[...] * freq_ref[...]
    cos = jnp.cos(ang)
    sin = jnp.sin(ang)
    lane = lax.broadcasted_iota(jnp.int32, (rows, HEAD), 1)
    even = (lane % 2) == 0
    sin = jnp.where(even, -sin, sin)

    def rot(v):
        swapped = jnp.where(even, pltpu.roll(v, HEAD - 1, 1), pltpu.roll(v, 1, 1))
        return v * cos + swapped * sin

    nxt = min(KV_AHEAD, nblk)
    bias = bq_ref[...].astype(jnp.float32).reshape(1, nq * qc)
    for c in range(nq):
        wq_copy(c).wait()
        if c + WQ_AHEAD < nq:
            wq_copy(c + WQ_AHEAD).start()
        if nxt < nblk and c + WQ_AHEAD >= nq - 1:
            for cp in kv_in(nxt):
                cp.start()
            nxt += 1
        out = jnp.dot(n_s[...], wq[:, c * qc:(c + 1) * qc], preferred_element_type=jnp.float32)
        out = out + bias[:, c * qc:(c + 1) * qc]
        for t in range(qc // HEAD):
            hh = c * (qc // HEAD) + t
            part = out[:, t * HEAD:(t + 1) * HEAD]
            if hh < heads:
                q_s[pl.ds(hh, rows, stride=heads), :] = rot(part)
            elif hh < heads + groups:
                kn_s[pl.ds(hh - heads, rows, stride=groups), :] = rot(part)
            else:
                vn_s[pl.ds(hh - heads - groups, rows, stride=groups), :] = part
    while nxt < nblk:
        for cp in kv_in(nxt):
            cp.start()
        nxt += 1
    wp_copy.start()

    col = lax.broadcasted_iota(jnp.int32, (heads, keys), 1)
    row = lax.broadcasted_iota(jnp.int32, (heads, keys), 0)
    own = (col % groups) == (row // (heads // groups))
    pos = jnp.where(own, col // groups, keys)
    r16 = lax.broadcasted_iota(jnp.int32, (16, HEAD), 0)
    r_pos = r16 // groups
    r_first = (r16 % groups) == 0
    zero = jnp.zeros((heads, HEAD), jnp.bfloat16)

    def insert(buf, new_s, b, length):
        base = pl.multiple_of((length // 8) * 16, 16)
        old = buf[b, pl.ds(base, 16), :]
        new = jnp.where(r_first, new_s[pl.ds(2 * b, 1), :], new_s[pl.ds(2 * b + 1, 1), :])
        buf[b, pl.ds(base, 16), :] = jnp.where(r_pos == length % 8, new, old.astype(jnp.float32)).astype(jnp.bfloat16)

    def scores(b):
        qa = q_s[pl.ds(b * heads, heads), :].astype(jnp.bfloat16)
        qb = q_s[pl.ds((b + 1) * heads, heads), :].astype(jnp.bfloat16)
        lhs = jnp.concatenate([jnp.concatenate([qa, zero], 1), jnp.concatenate([zero, qb], 1)], 0)
        rhs = jnp.concatenate([kbuf[b], kbuf[b + 1]], 1)
        return lax.dot_general(lhs, rhs, (((1,), (1,)), ((), ())), preferred_element_type=jnp.float32)

    def softmax(s, length):
        s = jnp.where(pos <= length, s * SCALE, -jnp.inf)
        p = jnp.exp(s - jnp.max(s, axis=-1, keepdims=True))
        return (p / jnp.sum(p, axis=-1, keepdims=True)).astype(jnp.bfloat16)

    def values(p, b):
        rhs = jnp.concatenate([vbuf[b], vbuf[b + 1]], 1)
        r = jnp.dot(p, rhs, preferred_element_type=jnp.float32)
        ctx_s[pl.ds(b * heads, heads), :] = r[:heads, :HEAD]
        ctx_s[pl.ds((b + 1) * heads, heads), :] = r[heads:, HEAD:]

    pairs = blk // 2

    def block(i, carry):
        for cp in kv_in(i):
            cp.wait()
        for j in range(blk):
            b = i * blk + j
            length = len_ref[b]
            insert(kbuf, kn_s, b, length)
            insert(vbuf, vn_s, b, length)
        for t in range(pairs):
            s_s[t] = scores(i * blk + 2 * t)
        for t in range(pairs):
            b = i * blk + 2 * t
            p_s[t, :heads, :] = softmax(s_s[t, :heads, :], len_ref[b])
            p_s[t, heads:, :] = softmax(s_s[t, heads:, :], len_ref[b + 1])
        for t in range(pairs):
            values(p_s[t], i * blk + 2 * t)
        for cp in kv_out(i):
            cp.start()
        return carry

    lax.fori_loop(0, nblk, block, 0)

    for h in range(heads):
        ctxb_s[:, h * HEAD:(h + 1) * HEAD] = ctx_s[pl.ds(h, rows, stride=heads), :].astype(jnp.bfloat16)
    wp_copy.wait()
    pc = 512
    for c in range(hid // pc):
        sl = slice(c * pc, (c + 1) * pc)
        hid_ref[:, sl] = x_ref[:, sl].astype(jnp.float32) + jnp.dot(
            ctxb_s[...], wp[:, sl], preferred_element_type=jnp.float32)
    h32 = hid_ref[...]
    ms = jnp.mean(h32 * h32, axis=-1, keepdims=True)
    m_ref[...] = (h32 * lax.rsqrt(ms + EPS) * gm_ref[...].astype(jnp.float32).reshape(1, hid)).astype(jnp.bfloat16)

    def drain(i, carry):
        for cp in kv_out(i):
            cp.wait()
        return carry

    lax.fori_loop(0, nblk, drain, 0)


def attention(x, lens, kc, vc, ga, wqkv, bqkv, wproj, gm):
    rows, hid = x.shape
    cache_len, groups = kc.shape[1], kc.shape[2]
    heads = wproj.shape[0] // HEAD
    blk, qc = 8, 256
    nblk = rows // blk
    freq = np.zeros((1, HEAD), np.float32)
    freq[0, :ROT] = np.repeat(np.float32(10000.0) ** (-np.arange(0, ROT, 2, dtype=np.float32) / np.float32(ROT)), 2)
    keys = cache_len * groups
    kflat = kc.reshape(rows, keys, HEAD)
    vflat = vc.reshape(rows, keys, HEAD)
    vm = pl.BlockSpec(memory_space=pltpu.VMEM)
    hbm = pl.BlockSpec(memory_space=pl.ANY)
    bf, f32 = jnp.bfloat16, jnp.float32
    dma = pltpu.SemaphoreType.DMA
    hidden, m, ko, vo = pl.pallas_call(
        functools.partial(attn_kernel, rows=rows, blk=blk, heads=heads, groups=groups, qc=qc),
        name="attn",
        out_shape=(pltpu.VMEM((rows, hid), f32), pltpu.VMEM((rows, hid), bf),
                   jax.ShapeDtypeStruct(kflat.shape, bf), jax.ShapeDtypeStruct(vflat.shape, bf)),
        in_specs=[hbm] * 10,
        out_specs=(vm, vm, hbm, hbm),
        scratch_shapes=[
            pltpu.VMEM((rows, keys, HEAD), bf), pltpu.VMEM((rows, keys, HEAD), bf),
            pltpu.VMEM(wqkv.shape, bf), pltpu.VMEM(wproj.shape, bf),
            pltpu.SMEM((rows,), jnp.int32), pltpu.VMEM((1, HEAD), f32), pltpu.VMEM((rows, hid), bf),
            pltpu.VMEM(ga.shape, bf), pltpu.VMEM(bqkv.shape, bf), pltpu.VMEM(gm.shape, bf),
            pltpu.VMEM((rows, hid), bf), pltpu.VMEM((rows, HEAD), f32),
            pltpu.VMEM((rows * heads, HEAD), f32),
            pltpu.VMEM((rows * groups, HEAD), f32), pltpu.VMEM((rows * groups, HEAD), f32),
            pltpu.VMEM((blk // 2, 2 * heads, keys), f32), pltpu.VMEM((blk // 2, 2 * heads, keys), bf),
            pltpu.VMEM((rows * heads, HEAD), f32), pltpu.VMEM((rows, heads * HEAD), bf),
            dma((6,)), dma((wqkv.shape[1] // qc,)), dma(()),
            dma((nblk,)), dma((nblk,)), dma((nblk,)), dma((nblk,)),
        ],
        compiler_params=pltpu.CompilerParams(vmem_limit_bytes=60 * 1024 * 1024),
        cost_estimate=pl.CostEstimate(flops=2 * rows * hid * 4608 + 4 * rows * heads * keys * HEAD,
                                      bytes_accessed=86000000, transcendentals=rows * heads * keys),
    )(lens, jnp.asarray(freq), x, ga, wqkv, bqkv, wproj, gm, kflat, vflat)
    return hidden, m, ko.reshape(kc.shape), vo.reshape(vc.shape)


def mlp_kernel(hid_ref, m_ref, wi_hbm, wo_hbm, out_ref,
               wi, wt, wo, gath, act, own_s, ps, rb, sb, rr,
               wi_sem, wt_sem, wo_sem, ag_send, ag_recv, fw_send, ps_send, ps_recv, rs_send, rs_recv,
               *, chunks, crows, full, tail, fc, nc):
    hid = m_ref.shape[1]
    ncol = hid // nc
    me = lax.axis_index('grp')
    core, xx, yy = me % 2, (me // 2) % 2, me // 4
    peer = me + 1 - 2 * core
    near_x = me + 2 - 4 * xx
    near_y = me + 4 - 8 * yy
    diag = me + 2 - 4 * xx + 4 - 8 * yy
    remote = (near_x, near_y, diag)

    def wi_copy(f, g):
        sl = pl.ds(f * fc, fc)
        return pltpu.make_async_copy(wi_hbm.at[g, sl], wi.at[g, sl], wi_sem.at[f, g])

    def wt_copy(g):
        return pltpu.make_async_copy(wi_hbm.at[g, pl.ds(full * fc, tail)], wt.at[pl.ds(g * (fc // 2), tail)], wt_sem.at[g])

    def wo_copy(c):
        return pltpu.make_async_copy(wo_hbm.at[:, pl.ds(c * nc, nc)],
                                     wo.at[pl.ds(0, full * fc + tail), pl.ds(c * nc, nc)], wo_sem.at[c])

    for f in range(full):
        for g in range(2):
            wi_copy(f, g).start()
    for g in range(2):
        wt_copy(g).start()
    for c in range(ncol):
        wo_copy(c).start()

    def rcopy(src, dst, ss, rs, dev):
        return pltpu.make_async_remote_copy(src_ref=src, dst_ref=dst, send_sem=ss, recv_sem=rs,
                                            device_id={'grp': dev}, device_id_type=pl.DeviceIdType.MESH)

    def own_send(h, q):
        slot, dev = ((4, peer), (1, near_x), (2, near_y), (3, diag))[q]
        return rcopy(m_ref.at[pl.ds(h * crows, crows)], gath.at[h, pl.ds(slot * crows, crows)],
                     ag_send.at[h, q], ag_recv.at[h, slot], dev)

    def forward(h, q):
        return rcopy(gath.at[h, pl.ds(q * crows, crows)], gath.at[h, pl.ds((q + 4) * crows, crows)],
                     fw_send.at[h, q], ag_recv.at[h, q + 4], peer)

    def pair_send(h, c):
        sl = (h, slice(None), pl.ds(c * nc, nc))
        return rcopy(ps.at[sl], rb.at[sl], ps_send.at[h, c], ps_recv.at[h, c], peer)

    def part_send(h, c, q):
        sl = (h, q, slice(None), pl.ds(c * nc, nc))
        return rcopy(sb.at[sl], rr.at[sl], rs_send.at[h, c, q], rs_recv.at[h, c, q], remote[q])

    barrier = pltpu.get_barrier_semaphore()
    for dev in (peer,) + remote:
        pl.semaphore_signal(barrier, inc=1, device_id={'grp': dev}, device_id_type=pl.DeviceIdType.MESH)
    pl.semaphore_wait(barrier, 4)

    for h in range(chunks):
        for q in (1, 2, 3, 0):
            own_send(h, q).start()

    pad = fc // 2 - tail
    for g in range(2):
        wt[g * (fc // 2) + tail:(g + 1) * (fc // 2), :] = jnp.zeros((pad, hid), jnp.bfloat16)
    wo[full * fc + tail:, :] = jnp.zeros((pad, hid), jnp.bfloat16)
    for h in range(chunks):
        gath[h, 0:crows] = m_ref[h * crows:(h + 1) * crows, :]

    nt = (((1,), (1,)), ((), ()))

    def pair_sum(h, c):
        pair_send(h, c).wait_recv()
        cs = slice(c * nc, (c + 1) * nc)
        tot = own_s[h, :, cs] + rb[h, :, cs].astype(jnp.float32)
        own_s[h, 0:crows, cs] = tot[0:crows]
        for q in range(3):
            sb[h, q, :, cs] = tot[(q + 1) * crows:(q + 2) * crows].astype(jnp.bfloat16)
        for q in (2, 0, 1):
            part_send(h, c, q).start()

    for h in range(chunks):
        for q in (1, 2, 3):
            own_send(h, q).wait_recv()
            forward(h, q).start()
        own_send(h, 0).wait_recv()
        for q in (1, 2, 3):
            forward(h, q).wait_recv()

        def in_proj(f, carry):
            if h == 0:
                for g in range(2):
                    wi_copy(f, g).wait()
            sl = pl.ds(pl.multiple_of(f * fc, fc), fc)
            gate = lax.dot_general(gath[h], wi[0, sl, :], nt, preferred_element_type=jnp.float32)
            up = lax.dot_general(gath[h], wi[1, sl, :], nt, preferred_element_type=jnp.float32)
            act[:, sl] = (jax.nn.silu(gate) * up).astype(jnp.bfloat16)
            return carry

        lax.fori_loop(0, full, in_proj, 0)
        if h == 0:
            for g in range(2):
                wt_copy(g).wait()
        gu = lax.dot_general(gath[h], wt[...], nt, preferred_element_type=jnp.float32)
        act[:, full * fc:] = (jax.nn.silu(gu[:, :fc // 2]) * gu[:, fc // 2:]).astype(jnp.bfloat16)

        half = 4 * crows
        for c in range(ncol):
            if h == 0:
                wo_copy(c).wait()
            cs = slice(c * nc, (c + 1) * nc)
            part = jnp.dot(act[...], wo[:, cs], preferred_element_type=jnp.float32)
            ps[h, :, cs] = part[half:].astype(jnp.bfloat16)
            own_s[h, :, cs] = part[:half]
            pair_send(h, c).start()
            if c > 0:
                pair_sum(h, c - 1)
        pair_sum(h, ncol - 1)

    for h in range(chunks):
        rs = slice(h * crows, (h + 1) * crows)
        for c in range(ncol):
            cs = slice(c * nc, (c + 1) * nc)
            for q in range(3):
                part_send(h, c, q).wait_recv()
            tot = hid_ref[rs, cs] + own_s[h, 0:crows, cs]
            for q in range(3):
                tot = tot + rr[h, q, :, cs].astype(jnp.float32)
            out_ref[rs, cs] = tot.astype(jnp.bfloat16)

    for h in range(chunks):
        for q in range(4):
            own_send(h, q).wait_send()
        for q in (1, 2, 3):
            forward(h, q).wait_send()
        for c in range(ncol):
            pair_send(h, c).wait_send()
            for q in range(3):
                part_send(h, c, q).wait_send()


def mlp(hidden, m, w_in, w_out):
    rows, hid = m.shape
    ffn = w_out.shape[0]
    chunks, fc, nc = 2, 256, 512
    crows = rows // chunks
    full, tail = ffn // fc, ffn % fc
    ncol = hid // nc
    vm = pl.BlockSpec(memory_space=pltpu.VMEM)
    hbm = pl.BlockSpec(memory_space=pl.ANY)
    bf, f32 = jnp.bfloat16, jnp.float32
    dma = pltpu.SemaphoreType.DMA
    return pl.pallas_call(
        functools.partial(mlp_kernel, chunks=chunks, crows=crows, full=full, tail=tail, fc=fc, nc=nc),
        name="mlp",
        out_shape=jax.ShapeDtypeStruct((rows, hid), bf),
        in_specs=[vm, vm, hbm, hbm],
        out_specs=vm,
        scratch_shapes=[
            pltpu.VMEM((2, full * fc, hid), bf), pltpu.VMEM((fc, hid), bf), pltpu.VMEM((full * fc + fc // 2, hid), bf),
            pltpu.VMEM((chunks, 8 * crows, hid), bf), pltpu.VMEM((8 * crows, full * fc + fc // 2), bf),
            pltpu.VMEM((chunks, 4 * crows, hid), f32), pltpu.VMEM((chunks, 4 * crows, hid), bf),
            pltpu.VMEM((chunks, 4 * crows, hid), bf),
            pltpu.VMEM((chunks, 3, crows, hid), bf), pltpu.VMEM((chunks, 3, crows, hid), bf),
            dma((full, 2)), dma((2,)), dma((ncol,)),
            dma((chunks, 4)), dma((chunks, 8)), dma((chunks, 4)),
            dma((chunks, ncol)), dma((chunks, ncol)), dma((chunks, ncol, 3)), dma((chunks, ncol, 3)),
        ],
        compiler_params=pltpu.CompilerParams(collective_id=0, has_side_effects=True, vmem_limit_bytes=34 << 20),
        cost_estimate=pl.CostEstimate(flops=2 * 8 * rows * hid * ffn * 3, bytes_accessed=17000000, transcendentals=8 * rows * ffn),
    )(pltpu.with_memory_space_constraint(hidden, pltpu.VMEM), pltpu.with_memory_space_constraint(m, pltpu.VMEM),
      pltpu.with_memory_space_constraint(w_in, pltpu.HBM), pltpu.with_memory_space_constraint(w_out, pltpu.HBM))


def solution(mesh):
    row_spec = P(('rep', 'grp'))
    repl_spec = P()

    def local_layer(x_in, seq_len, k_cache, v_cache, gamma_attn, w_qkv, b_qkv, w_proj, gamma_mlp, w_in, w_out):
        hidden, mlp_in, k_out, v_out = attention(x_in, seq_len, k_cache, v_cache, gamma_attn, w_qkv, b_qkv, w_proj, gamma_mlp)
        layer_out = mlp(hidden, mlp_in, w_in, w_out)
        return layer_out, k_out, v_out

    return jax.shard_map(local_layer, mesh=mesh,
                         in_specs=(row_spec, row_spec, row_spec, row_spec, repl_spec, repl_spec, repl_spec,
                                   repl_spec, repl_spec, P(None, 'grp', None), P('grp', None)),
                         out_specs=(row_spec, row_spec, row_spec), check_vma=False)
```

```python
import functools
import jax
import jax.numpy as jnp
import numpy as np
from jax import lax
from jax.experimental import pallas as pl
from jax.experimental.pallas import tpu as pltpu
from jax.sharding import PartitionSpec as P

HEAD = 128
ROT = 64
EPS = 1e-5
SCALE = HEAD ** -0.5
WQ_AHEAD = 10
KV_AHEAD = 4


def attn_kernel(len_hbm, freq_hbm, x_hbm, ga_hbm, wq_hbm, bq_hbm, wp_hbm, gm_hbm, kc_hbm, vc_hbm,
                hid_ref, m_ref, ko_hbm, vo_hbm,
                kbuf, vbuf, wq, wp, len_ref, freq_ref, x_ref, ga_ref, bq_ref, gm_ref,
                n_s, lens_s, q_s, kn_s, vn_s, s_s, p_s, ctx_s, ctxb_s,
                small_sem, wq_sem, wp_sem, kin_sem, vin_sem, kout_sem, vout_sem,
                *, rows, blk, heads, groups, qc):
    nblk = rows // blk
    hid = x_ref.shape[1]
    keys = kbuf.shape[1]
    nq = wq.shape[1] // qc

    small = [pltpu.make_async_copy(src, dst, small_sem.at[i]) for i, (src, dst) in enumerate((
        (x_hbm, x_ref), (len_hbm, len_ref), (ga_hbm, ga_ref), (freq_hbm, freq_ref),
        (bq_hbm, bq_ref), (gm_hbm, gm_ref)))]

    def wq_copy(c):
        return pltpu.make_async_copy(wq_hbm.at[:, pl.ds(c * qc, qc)], wq.at[:, pl.ds(c * qc, qc)], wq_sem.at[c])

    def kv_in(i):
        sl = pl.ds(i * blk, blk)
        return (pltpu.make_async_copy(kc_hbm.at[sl], kbuf.at[sl], kin_sem.at[i]),
                pltpu.make_async_copy(vc_hbm.at[sl], vbuf.at[sl], vin_sem.at[i]))

    def kv_out(i):
        sl = pl.ds(i * blk, blk)
        return (pltpu.make_async_copy(kbuf.at[sl], ko_hbm.at[sl], kout_sem.at[i]),
                pltpu.make_async_copy(vbuf.at[sl], vo_hbm.at[sl], vout_sem.at[i]))

    wp_copy = pltpu.make_async_copy(wp_hbm, wp, wp_sem)

    for cp in small:
        cp.start()
    for c in range(min(WQ_AHEAD, nq)):
        wq_copy(c).start()
    for i in range(min(KV_AHEAD, nblk)):
        for cp in kv_in(i):
            cp.start()
    for cp in small:
        cp.wait()

    for b in range(rows):
        lens_s[pl.ds(b, 1), :] = jnp.full((1, HEAD), len_ref[b].astype(jnp.float32), jnp.float32)
    x32 = x_ref[...].astype(jnp.float32)
    ms = jnp.mean(x32 * x32, axis=-1, keepdims=True)
    n_s[...] = (x32 * lax.rsqrt(ms + EPS) * ga_ref[...].astype(jnp.float32).reshape(1, hid)).astype(jnp.bfloat16)
    ang = lens_s[...] * freq_ref[...]
    cos = jnp.cos(ang)
    sin = jnp.sin(ang)
    lane = lax.broadcasted_iota(jnp.int32, (rows, HEAD), 1)
    even = (lane % 2) == 0
    sin = jnp.where(even, -sin, sin)

    def rot(v):
        swapped = jnp.where(even, pltpu.roll(v, HEAD - 1, 1), pltpu.roll(v, 1, 1))
        return v * cos + swapped * sin

    nxt = min(KV_AHEAD, nblk)
    bias = bq_ref[...].astype(jnp.float32).reshape(1, nq * qc)
    for c in range(nq):
        wq_copy(c).wait()
        if c + WQ_AHEAD < nq:
            wq_copy(c + WQ_AHEAD).start()
        if nxt < nblk and c + WQ_AHEAD >= nq - 1:
            for cp in kv_in(nxt):
                cp.start()
            nxt += 1
        out = jnp.dot(n_s[...], wq[:, c * qc:(c + 1) * qc], preferred_element_type=jnp.float32)
        out = out + bias[:, c * qc:(c + 1) * qc]
        for t in range(qc // HEAD):
            hh = c * (qc // HEAD) + t
            part = out[:, t * HEAD:(t + 1) * HEAD]
            if hh < heads:
                q_s[pl.ds(hh, rows, stride=heads), :] = rot(part)
            elif hh < heads + groups:
                kn_s[pl.ds(hh - heads, rows, stride=groups), :] = rot(part)
            else:
                vn_s[pl.ds(hh - heads - groups, rows, stride=groups), :] = part
    while nxt < nblk:
        for cp in kv_in(nxt):
            cp.start()
        nxt += 1
    wp_copy.start()

    col = lax.broadcasted_iota(jnp.int32, (heads, keys), 1)
    row = lax.broadcasted_iota(jnp.int32, (heads, keys), 0)
    own = (col % groups) == (row // (heads // groups))
    pos = jnp.where(own, col // groups, keys)
    r16 = lax.broadcasted_iota(jnp.int32, (16, HEAD), 0)
    r_pos = r16 // groups
    r_first = (r16 % groups) == 0
    zero = jnp.zeros((heads, HEAD), jnp.bfloat16)

    def insert(buf, new_s, b, length):
        base = pl.multiple_of((length // 8) * 16, 16)
        old = buf[b, pl.ds(base, 16), :]
        new = jnp.where(r_first, new_s[pl.ds(2 * b, 1), :], new_s[pl.ds(2 * b + 1, 1), :])
        buf[b, pl.ds(base, 16), :] = jnp.where(r_pos == length % 8, new, old.astype(jnp.float32)).astype(jnp.bfloat16)

    def scores(b):
        qa = q_s[pl.ds(b * heads, heads), :].astype(jnp.bfloat16)
        qb = q_s[pl.ds((b + 1) * heads, heads), :].astype(jnp.bfloat16)
        lhs = jnp.concatenate([jnp.concatenate([qa, zero], 1), jnp.concatenate([zero, qb], 1)], 0)
        rhs = jnp.concatenate([kbuf[b], kbuf[b + 1]], 1)
        return lax.dot_general(lhs, rhs, (((1,), (1,)), ((), ())), preferred_element_type=jnp.float32)

    def softmax(s, length):
        s = jnp.where(pos <= length, s * SCALE, -jnp.inf)
        p = jnp.exp(s - jnp.max(s, axis=-1, keepdims=True))
        return (p / jnp.sum(p, axis=-1, keepdims=True)).astype(jnp.bfloat16)

    def values(p, b):
        rhs = jnp.concatenate([vbuf[b], vbuf[b + 1]], 1)
        r = jnp.dot(p, rhs, preferred_element_type=jnp.float32)
        ctx_s[pl.ds(b * heads, heads), :] = r[:heads, :HEAD]
        ctx_s[pl.ds((b + 1) * heads, heads), :] = r[heads:, HEAD:]

    pairs = blk // 2

    def block(i, carry):
        for cp in kv_in(i):
            cp.wait()
        for j in range(blk):
            b = i * blk + j
            length = len_ref[b]
            insert(kbuf, kn_s, b, length)
            insert(vbuf, vn_s, b, length)
        for t in range(pairs):
            s_s[t] = scores(i * blk + 2 * t)
        for t in range(pairs):
            b = i * blk + 2 * t
            p_s[t, :heads, :] = softmax(s_s[t, :heads, :], len_ref[b])
            p_s[t, heads:, :] = softmax(s_s[t, heads:, :], len_ref[b + 1])
        for t in range(pairs):
            values(p_s[t], i * blk + 2 * t)
        for cp in kv_out(i):
            cp.start()
        return carry

    lax.fori_loop(0, nblk, block, 0)

    for h in range(heads):
        ctxb_s[:, h * HEAD:(h + 1) * HEAD] = ctx_s[pl.ds(h, rows, stride=heads), :].astype(jnp.bfloat16)
    wp_copy.wait()
    pc = 512
    for c in range(hid // pc):
        sl = slice(c * pc, (c + 1) * pc)
        hid_ref[:, sl] = x_ref[:, sl].astype(jnp.float32) + jnp.dot(
            ctxb_s[...], wp[:, sl], preferred_element_type=jnp.float32)
    h32 = hid_ref[...]
    ms = jnp.mean(h32 * h32, axis=-1, keepdims=True)
    m_ref[...] = (h32 * lax.rsqrt(ms + EPS) * gm_ref[...].astype(jnp.float32).reshape(1, hid)).astype(jnp.bfloat16)

    def drain(i, carry):
        for cp in kv_out(i):
            cp.wait()
        return carry

    lax.fori_loop(0, nblk, drain, 0)


def attention(x, lens, kc, vc, ga, wqkv, bqkv, wproj, gm):
    rows, hid = x.shape
    cache_len, groups = kc.shape[1], kc.shape[2]
    heads = wproj.shape[0] // HEAD
    blk, qc = 8, 256
    nblk = rows // blk
    freq = np.zeros((1, HEAD), np.float32)
    freq[0, :ROT] = np.repeat(np.float32(10000.0) ** (-np.arange(0, ROT, 2, dtype=np.float32) / np.float32(ROT)), 2)
    keys = cache_len * groups
    kflat = kc.reshape(rows, keys, HEAD)
    vflat = vc.reshape(rows, keys, HEAD)
    vm = pl.BlockSpec(memory_space=pltpu.VMEM)
    hbm = pl.BlockSpec(memory_space=pl.ANY)
    bf, f32 = jnp.bfloat16, jnp.float32
    dma = pltpu.SemaphoreType.DMA
    hidden, m, ko, vo = pl.pallas_call(
        functools.partial(attn_kernel, rows=rows, blk=blk, heads=heads, groups=groups, qc=qc),
        name="attn",
        out_shape=(pltpu.VMEM((rows, hid), f32), pltpu.VMEM((rows, hid), bf),
                   jax.ShapeDtypeStruct(kflat.shape, bf), jax.ShapeDtypeStruct(vflat.shape, bf)),
        in_specs=[hbm] * 10,
        out_specs=(vm, vm, hbm, hbm),
        scratch_shapes=[
            pltpu.VMEM((rows, keys, HEAD), bf), pltpu.VMEM((rows, keys, HEAD), bf),
            pltpu.VMEM(wqkv.shape, bf), pltpu.VMEM(wproj.shape, bf),
            pltpu.SMEM((rows,), jnp.int32), pltpu.VMEM((1, HEAD), f32), pltpu.VMEM((rows, hid), bf),
            pltpu.VMEM(ga.shape, bf), pltpu.VMEM(bqkv.shape, bf), pltpu.VMEM(gm.shape, bf),
            pltpu.VMEM((rows, hid), bf), pltpu.VMEM((rows, HEAD), f32),
            pltpu.VMEM((rows * heads, HEAD), f32),
            pltpu.VMEM((rows * groups, HEAD), f32), pltpu.VMEM((rows * groups, HEAD), f32),
            pltpu.VMEM((blk // 2, 2 * heads, keys), f32), pltpu.VMEM((blk // 2, 2 * heads, keys), bf),
            pltpu.VMEM((rows * heads, HEAD), f32), pltpu.VMEM((rows, heads * HEAD), bf),
            dma((6,)), dma((wqkv.shape[1] // qc,)), dma(()),
            dma((nblk,)), dma((nblk,)), dma((nblk,)), dma((nblk,)),
        ],
        compiler_params=pltpu.CompilerParams(vmem_limit_bytes=60 * 1024 * 1024),
        cost_estimate=pl.CostEstimate(flops=2 * rows * hid * 4608 + 4 * rows * heads * keys * HEAD,
                                      bytes_accessed=86000000, transcendentals=rows * heads * keys),
    )(lens, jnp.asarray(freq), x, ga, wqkv, bqkv, wproj, gm, kflat, vflat)
    return hidden, m, ko.reshape(kc.shape), vo.reshape(vc.shape)


def mlp_kernel(hid_ref, m_ref, wi_hbm, wo_hbm, out_ref,
               wi, wt, wtr, wo, chip, gath, act, own_s, part_s, cps, crb, ps, rb, sb, t1, rr,
               wi_sem, wt_sem, wo_sem, peer_send, peer_recv, near_send, near_recv, rel_send, rel_recv,
               fw_send, fw_recv, cp_send, cp_recv, ps_send, ps_recv, rs_send, t1_recv, rr_recv,
               *, chunks, full, tail, fc, nc):
    rows, hid = m_ref.shape
    crows = rows // chunks
    half = crows // 2
    ncol = hid // nc
    width = full * fc + fc // 2
    bf, f32 = jnp.bfloat16, jnp.float32
    me = lax.axis_index('grp')
    core, xx, yy = me % 2, (me // 2) % 2, me // 4
    peer = me + 1 - 2 * core
    near = (me + 2 - 4 * xx, me + 4 - 8 * yy)

    def wi_copy(f, g):
        sl = pl.ds(f * fc, fc)
        return pltpu.make_async_copy(wi_hbm.at[g, sl], wi.at[g, sl], wi_sem.at[f, g])

    def wt_copy(g):
        return pltpu.make_async_copy(wi_hbm.at[g, pl.ds(full * fc, tail)], wt.at[g, pl.ds(0, tail)], wt_sem.at[g])

    wo_copy = pltpu.make_async_copy(wo_hbm, wo.at[pl.ds(0, full * fc + tail)], wo_sem)

    for f in range(full):
        for g in range(2):
            wi_copy(f, g).start()
    for g in range(2):
        wt_copy(g).start()
    wo_copy.start()

    def rcopy(src, dst, ss, rs, dev):
        return pltpu.make_async_remote_copy(src_ref=src, dst_ref=dst, send_sem=ss, recv_sem=rs,
                                            device_id={'grp': dev}, device_id_type=pl.DeviceIdType.MESH)

    def g_at(h, slot, p=None):
        if p is None:
            return gath.at[h, pl.ds(slot * crows, crows)]
        return gath.at[h, pl.ds(slot * crows + p * half, half)]

    to_peer = rcopy(m_ref, chip.at[pl.ds(rows, rows)], peer_send, peer_recv, peer)

    def to_near(h, d, p):
        return rcopy(m_ref.at[pl.ds(h * crows + p * half, half)], g_at(h, d, p),
                     near_send.at[h, d, p], near_recv.at[h, d, p], near[d])

    def relay(h, d):
        return rcopy(g_at(h, d, d), g_at(h, 2, d), rel_send.at[h, d], rel_recv.at[h, d], near[1 - d])

    def forward(h, s):
        return rcopy(g_at(h, s), g_at(h, 3 + s), fw_send.at[h, s], fw_recv.at[h, s], peer)

    def cols(c):
        return slice(c * nc, (c + 1) * nc)

    def chip_send(c):
        sl = (slice(None), pl.ds(c * nc, nc))
        return rcopy(cps.at[sl], crb.at[sl], cp_send.at[c], cp_recv.at[c], peer)

    def pair_send(h, c):
        sl = (h, slice(None), pl.ds(c * nc, nc))
        return rcopy(ps.at[sl], rb.at[sl], ps_send.at[h, c], ps_recv.at[h, c], peer)

    def diag_send(h, c, d):
        sl = (h, d, slice(None), pl.ds(c * nc, nc))
        return rcopy(sb.at[sl], t1.at[sl], rs_send.at[h, c, d], t1_recv.at[h, c, d], near[d])

    def near_part(h, c, d, p):
        k = 2 + 2 * d + p
        return rcopy(sb.at[h, k, :, pl.ds(c * nc, nc)], rr.at[h, d, p, :, pl.ds(c * nc, nc)],
                     rs_send.at[h, c, k], rr_recv.at[h, c, d, p], near[d])

    barrier = pltpu.get_barrier_semaphore()
    for dev in (peer,) + near:
        pl.semaphore_signal(barrier, inc=1, device_id={'grp': dev}, device_id_type=pl.DeviceIdType.MESH)
    pl.semaphore_wait(barrier, 3)

    def send_own(h):
        for p in range(2):
            for d in range(2):
                to_near(h, d, p if d == 0 else 1 - p).start()

    def pass_on(h):
        for d in range(2):
            to_near(h, d, d).wait_recv()
            relay(h, d).start()

    def share(h):
        for d in range(2):
            to_near(h, d, 1 - d).wait_recv()
            forward(h, d).start()

    def share_diag(h):
        for d in range(2):
            relay(h, d).wait_recv()
        forward(h, 2).start()

    def all_here(h):
        for s in range(3):
            forward(h, s).wait_recv()

    to_peer.start()
    send_own(0)
    for g in range(2):
        wt[g, tail:, :] = jnp.zeros((fc // 2 - tail, hid), bf)
    wo[full * fc + tail:, :] = jnp.zeros((fc // 2 - tail, hid), bf)
    chip[0:rows] = m_ref[...]
    to_peer.wait_recv()

    def gated(gate, up):
        return (jax.nn.silu(gate) * up).astype(bf)

    nt = (((1,), (1,)), ((), ()))
    for f in range(full + 1):
        n = fc if f < full else fc // 2
        sl = slice(f * fc, f * fc + n)
        for g in range(2):
            (wi_copy(f, g) if f < full else wt_copy(g)).wait()
        raw = [wi[g, sl, :] if f < full else wt[g] for g in range(2)]
        gu = [lax.dot_general(chip[...], w, nt, preferred_element_type=f32) for w in raw]
        for g in range(2):
            wtr[g, :, sl] = raw[g].T
        act[0:2 * rows, sl] = gated(gu[0], gu[1])
        if f == HOOK_PASS:
            pass_on(0)
            send_own(1)
        if f == HOOK_SHARE:
            share(0)
    wo_copy.wait()
    for c in range(ncol):
        part = jnp.dot(act[0:2 * rows, :], wo[:, cols(c)], preferred_element_type=f32)
        cps[:, cols(c)] = part[rows:].astype(bf)
        own_s[:, cols(c)] = part[:rows]
        chip_send(c).start()

    def in_proj(h):
        for lo, hi in IN_CUTS:
            gate = jnp.dot(gath[h], wtr[0, :, lo:hi], preferred_element_type=f32)
            up = jnp.dot(gath[h], wtr[1, :, lo:hi], preferred_element_type=f32)
            act[0:6 * crows, lo:hi] = gated(gate, up)

    def out_proj(h):
        for c in range(ncol):
            part = jnp.dot(act[0:6 * crows, :], wo[:, cols(c)], preferred_element_type=f32)
            ps[h, :, cols(c)] = part[3 * crows:].astype(bf)
            part_s[h, :, cols(c)] = part[:3 * crows]
            pair_send(h, c).start()

    def stage1(h, c):
        pair_send(h, c).wait_recv()
        tot = part_s[h, :, cols(c)] + rb[h, :, cols(c)].astype(f32)
        part_s[h, 0:2 * crows, cols(c)] = tot[0:2 * crows]
        for d in range(2):
            r = 2 * crows + d * half
            sb[h, d, :, cols(c)] = tot[r:r + half].astype(bf)
            r = d * crows + d * half
            sb[h, 2 + 2 * d + d, :, cols(c)] = tot[r:r + half].astype(bf)
        for d in range(2):
            diag_send(h, c, d).start()
        for d in range(2):
            near_part(h, c, d, d).start()

    def stage2(h, c):
        for d in range(2):
            e = 1 - d
            diag_send(h, c, d).wait_recv()
            r = e * crows + d * half
            sb[h, 2 + 2 * e + d, :, cols(c)] = (part_s[h, r:r + half, cols(c)] + t1[h, d, :, cols(c)].astype(f32)).astype(bf)
            near_part(h, c, e, d).start()

    def chip_sum(c):
        chip_send(c).wait_recv()
        own_s[:, cols(c)] = hid_ref[:, cols(c)] + own_s[:, cols(c)] + crb[:, cols(c)].astype(f32)

    def finish(h, c):
        for d in range(2):
            for p in range(2):
                near_part(h, c, d, p).wait_recv()
        rs = slice(h * crows, (h + 1) * crows)
        tot = own_s[rs, cols(c)]
        for d in range(2):
            tot = tot + rr[h, d, :, :, cols(c)].reshape(crows, nc).astype(f32)
        out_ref[rs, cols(c)] = tot.astype(bf)

    share_diag(0)
    pass_on(1)
    for c in range(ncol):
        chip_sum(c)
    all_here(0)
    in_proj(0)
    share(1)
    out_proj(0)
    share_diag(1)
    for c in range(ncol):
        stage1(0, c)
    all_here(1)
    in_proj(1)
    out_proj(1)
    for c in range(ncol):
        stage2(0, c)
    for c in range(ncol):
        stage1(1, c)
    for c in range(ncol):
        finish(0, c)
    for c in range(ncol):
        stage2(1, c)
    for c in range(ncol):
        finish(1, c)

    to_peer.wait_send()
    for c in range(ncol):
        chip_send(c).wait_send()
    for h in range(chunks):
        for d in range(2):
            for p in range(2):
                to_near(h, d, p).wait_send()
            relay(h, d).wait_send()
        for s in range(3):
            forward(h, s).wait_send()
        for c in range(ncol):
            pair_send(h, c).wait_send()
            for d in range(2):
                diag_send(h, c, d).wait_send()
                for p in range(2):
                    near_part(h, c, d, p).wait_send()


HOOK_PASS = 2
HOOK_SHARE = 5
IN_CUTS = ((0, 512), (512, 1024), (1024, 1408))


def mlp(hidden, m, w_in, w_out):
    rows, hid = m.shape
    ffn = w_out.shape[0]
    chunks, fc, nc = 2, 256, 1024
    crows = rows // chunks
    half = crows // 2
    full, tail = ffn // fc, ffn % fc
    width = full * fc + fc // 2
    ncol = hid // nc
    vm = pl.BlockSpec(memory_space=pltpu.VMEM)
    hbm = pl.BlockSpec(memory_space=pl.ANY)
    bf, f32 = jnp.bfloat16, jnp.float32
    dma = pltpu.SemaphoreType.DMA
    return pl.pallas_call(
        functools.partial(mlp_kernel, chunks=chunks, full=full, tail=tail, fc=fc, nc=nc),
        name="mlp",
        out_shape=jax.ShapeDtypeStruct((rows, hid), bf),
        in_specs=[vm, vm, hbm, hbm],
        out_specs=vm,
        scratch_shapes=[
            pltpu.VMEM((2, full * fc, hid), bf), pltpu.VMEM((2, fc // 2, hid), bf), pltpu.VMEM((2, hid, width), bf),
            pltpu.VMEM((width, hid), bf),
            pltpu.VMEM((2 * rows, hid), bf), pltpu.VMEM((chunks, 6 * crows, hid), bf), pltpu.VMEM((6 * crows, width), bf),
            pltpu.VMEM((rows, hid), f32), pltpu.VMEM((chunks, 3 * crows, hid), f32),
            pltpu.VMEM((rows, hid), bf), pltpu.VMEM((rows, hid), bf),
            pltpu.VMEM((chunks, 3 * crows, hid), bf), pltpu.VMEM((chunks, 3 * crows, hid), bf),
            pltpu.VMEM((chunks, 6, half, hid), bf), pltpu.VMEM((chunks, 2, half, hid), bf),
            pltpu.VMEM((chunks, 2, 2, half, hid), bf),
            dma((full, 2)), dma((2,)), dma(()),
            dma(()), dma(()), dma((chunks, 2, 2)), dma((chunks, 2, 2)), dma((chunks, 2)), dma((chunks, 2)),
            dma((chunks, 3)), dma((chunks, 3)), dma((ncol,)), dma((ncol,)), dma((chunks, ncol)), dma((chunks, ncol)),
            dma((chunks, ncol, 6)), dma((chunks, ncol, 2)), dma((chunks, ncol, 2, 2)),
        ],
        compiler_params=pltpu.CompilerParams(collective_id=0, has_side_effects=True, vmem_limit_bytes=46 << 20),
        cost_estimate=pl.CostEstimate(flops=2 * 8 * rows * hid * ffn * 3, bytes_accessed=17000000, transcendentals=8 * rows * ffn),
    )(pltpu.with_memory_space_constraint(hidden, pltpu.VMEM), pltpu.with_memory_space_constraint(m, pltpu.VMEM),
      pltpu.with_memory_space_constraint(w_in, pltpu.HBM), pltpu.with_memory_space_constraint(w_out, pltpu.HBM))


def solution(mesh):
    row_spec = P(('rep', 'grp'))
    repl_spec = P()

    def local_layer(x_in, seq_len, k_cache, v_cache, gamma_attn, w_qkv, b_qkv, w_proj, gamma_mlp, w_in, w_out):
        hidden, mlp_in, k_out, v_out = attention(x_in, seq_len, k_cache, v_cache, gamma_attn, w_qkv, b_qkv, w_proj, gamma_mlp)
        layer_out = mlp(hidden, mlp_in, w_in, w_out)
        return layer_out, k_out, v_out

    return jax.shard_map(local_layer, mesh=mesh,
                         in_specs=(row_spec, row_spec, row_spec, row_spec, repl_spec, repl_spec, repl_spec,
                                   repl_spec, repl_spec, P(None, 'grp', None), P('grp', None)),
                         out_specs=(row_spec, row_spec, row_spec), check_vma=False)
```

```python
import functools
import jax
import jax.numpy as jnp
import numpy as np
from jax import lax
from jax.experimental import pallas as pl
from jax.experimental.pallas import tpu as pltpu
from jax.sharding import PartitionSpec as P

HEAD = 128
ROT = 64
EPS = 1e-5
SCALE = HEAD ** -0.5
WQ_AHEAD = 10
KV_AHEAD = 4


def attn_kernel(len_hbm, freq_hbm, x_hbm, ga_hbm, wq_hbm, bq_hbm, wp_hbm, gm_hbm, kc_hbm, vc_hbm,
                hid_ref, m_ref, ko_hbm, vo_hbm,
                kbuf, vbuf, wq, wp, len_ref, freq_ref, x_ref, ga_ref, bq_ref, gm_ref,
                n_s, lens_s, q_s, kn_s, vn_s, s_s, p_s, ctx_s, ctxb_s,
                small_sem, wq_sem, wp_sem, kin_sem, vin_sem, kout_sem, vout_sem,
                *, rows, blk, heads, groups, qc):
    nblk = rows // blk
    hid = x_ref.shape[1]
    keys = kbuf.shape[1]
    nq = wq.shape[1] // qc

    small = [pltpu.make_async_copy(src, dst, small_sem.at[i]) for i, (src, dst) in enumerate((
        (x_hbm, x_ref), (len_hbm, len_ref), (ga_hbm, ga_ref), (freq_hbm, freq_ref),
        (bq_hbm, bq_ref), (gm_hbm, gm_ref)))]

    def wq_copy(c):
        return pltpu.make_async_copy(wq_hbm.at[:, pl.ds(c * qc, qc)], wq.at[:, pl.ds(c * qc, qc)], wq_sem.at[c])

    def kv_in(i):
        sl = pl.ds(i * blk, blk)
        return (pltpu.make_async_copy(kc_hbm.at[sl], kbuf.at[sl], kin_sem.at[i]),
                pltpu.make_async_copy(vc_hbm.at[sl], vbuf.at[sl], vin_sem.at[i]))

    def kv_out(i):
        sl = pl.ds(i * blk, blk)
        return (pltpu.make_async_copy(kbuf.at[sl], ko_hbm.at[sl], kout_sem.at[i]),
                pltpu.make_async_copy(vbuf.at[sl], vo_hbm.at[sl], vout_sem.at[i]))

    wp_copy = pltpu.make_async_copy(wp_hbm, wp, wp_sem)

    for cp in small:
        cp.start()
    for c in range(min(WQ_AHEAD, nq)):
        wq_copy(c).start()
    for i in range(min(KV_AHEAD, nblk)):
        for cp in kv_in(i):
            cp.start()
    for cp in small:
        cp.wait()

    for b in range(rows):
        lens_s[pl.ds(b, 1), :] = jnp.full((1, HEAD), len_ref[b].astype(jnp.float32), jnp.float32)
    x32 = x_ref[...].astype(jnp.float32)
    ms = jnp.mean(x32 * x32, axis=-1, keepdims=True)
    n_s[...] = (x32 * lax.rsqrt(ms + EPS) * ga_ref[...].astype(jnp.float32).reshape(1, hid)).astype(jnp.bfloat16)
    ang = lens_s[...] * freq_ref[...]
    cos = jnp.cos(ang)
    sin = jnp.sin(ang)
    lane = lax.broadcasted_iota(jnp.int32, (rows, HEAD), 1)
    even = (lane % 2) == 0
    sin = jnp.where(even, -sin, sin)

    def rot(v):
        swapped = jnp.where(even, pltpu.roll(v, HEAD - 1, 1), pltpu.roll(v, 1, 1))
        return v * cos + swapped * sin

    nxt = min(KV_AHEAD, nblk)
    bias = bq_ref[...].astype(jnp.float32).reshape(1, nq * qc)
    for c in range(nq):
        wq_copy(c).wait()
        if c + WQ_AHEAD < nq:
            wq_copy(c + WQ_AHEAD).start()
        if nxt < nblk and c + WQ_AHEAD >= nq - 1:
            for cp in kv_in(nxt):
                cp.start()
            nxt += 1
        out = jnp.dot(n_s[...], wq[:, c * qc:(c + 1) * qc], preferred_element_type=jnp.float32)
        out = out + bias[:, c * qc:(c + 1) * qc]
        for t in range(qc // HEAD):
            hh = c * (qc // HEAD) + t
            part = out[:, t * HEAD:(t + 1) * HEAD]
            if hh < heads:
                q_s[pl.ds(hh, rows, stride=heads), :] = rot(part)
            elif hh < heads + groups:
                kn_s[pl.ds(hh - heads, rows, stride=groups), :] = rot(part)
            else:
                vn_s[pl.ds(hh - heads - groups, rows, stride=groups), :] = part
    while nxt < nblk:
        for cp in kv_in(nxt):
            cp.start()
        nxt += 1
    wp_copy.start()

    col = lax.broadcasted_iota(jnp.int32, (heads, keys), 1)
    row = lax.broadcasted_iota(jnp.int32, (heads, keys), 0)
    own = (col % groups) == (row // (heads // groups))
    pos = jnp.where(own, col // groups, keys)
    r16 = lax.broadcasted_iota(jnp.int32, (16, HEAD), 0)
    r_pos = r16 // groups
    r_first = (r16 % groups) == 0
    zero = jnp.zeros((heads, HEAD), jnp.bfloat16)

    def insert(buf, new_s, b, length):
        base = pl.multiple_of((length // 8) * 16, 16)
        old = buf[b, pl.ds(base, 16), :]
        new = jnp.where(r_first, new_s[pl.ds(2 * b, 1), :], new_s[pl.ds(2 * b + 1, 1), :])
        buf[b, pl.ds(base, 16), :] = jnp.where(r_pos == length % 8, new, old.astype(jnp.float32)).astype(jnp.bfloat16)

    def scores(b):
        qa = q_s[pl.ds(b * heads, heads), :].astype(jnp.bfloat16)
        qb = q_s[pl.ds((b + 1) * heads, heads), :].astype(jnp.bfloat16)
        lhs = jnp.concatenate([jnp.concatenate([qa, zero], 1), jnp.concatenate([zero, qb], 1)], 0)
        rhs = jnp.concatenate([kbuf[b], kbuf[b + 1]], 1)
        return lax.dot_general(lhs, rhs, (((1,), (1,)), ((), ())), preferred_element_type=jnp.float32)

    def softmax(s, length):
        s = jnp.where(pos <= length, s * SCALE, -jnp.inf)
        p = jnp.exp(s - jnp.max(s, axis=-1, keepdims=True))
        return (p / jnp.sum(p, axis=-1, keepdims=True)).astype(jnp.bfloat16)

    def values(p, b):
        rhs = jnp.concatenate([vbuf[b], vbuf[b + 1]], 1)
        r = jnp.dot(p, rhs, preferred_element_type=jnp.float32)
        ctx_s[pl.ds(b * heads, heads), :] = r[:heads, :HEAD]
        ctx_s[pl.ds((b + 1) * heads, heads), :] = r[heads:, HEAD:]

    pairs = blk // 2

    def block(i, carry):
        for cp in kv_in(i):
            cp.wait()
        for j in range(blk):
            b = i * blk + j
            length = len_ref[b]
            insert(kbuf, kn_s, b, length)
            insert(vbuf, vn_s, b, length)
        for t in range(pairs):
            s_s[t] = scores(i * blk + 2 * t)
        for t in range(pairs):
            b = i * blk + 2 * t
            p_s[t, :heads, :] = softmax(s_s[t, :heads, :], len_ref[b])
            p_s[t, heads:, :] = softmax(s_s[t, heads:, :], len_ref[b + 1])
        for t in range(pairs):
            values(p_s[t], i * blk + 2 * t)
        for cp in kv_out(i):
            cp.start()
        return carry

    lax.fori_loop(0, nblk, block, 0)

    for h in range(heads):
        ctxb_s[:, h * HEAD:(h + 1) * HEAD] = ctx_s[pl.ds(h, rows, stride=heads), :].astype(jnp.bfloat16)
    wp_copy.wait()
    pc = 512
    for c in range(hid // pc):
        sl = slice(c * pc, (c + 1) * pc)
        hid_ref[:, sl] = x_ref[:, sl].astype(jnp.float32) + jnp.dot(
            ctxb_s[...], wp[:, sl], preferred_element_type=jnp.float32)
    h32 = hid_ref[...]
    ms = jnp.mean(h32 * h32, axis=-1, keepdims=True)
    m_ref[...] = (h32 * lax.rsqrt(ms + EPS) * gm_ref[...].astype(jnp.float32).reshape(1, hid)).astype(jnp.bfloat16)

    def drain(i, carry):
        for cp in kv_out(i):
            cp.wait()
        return carry

    lax.fori_loop(0, nblk, drain, 0)


def attention(x, lens, kc, vc, ga, wqkv, bqkv, wproj, gm):
    rows, hid = x.shape
    cache_len, groups = kc.shape[1], kc.shape[2]
    heads = wproj.shape[0] // HEAD
    blk, qc = 8, 256
    nblk = rows // blk
    freq = np.zeros((1, HEAD), np.float32)
    freq[0, :ROT] = np.repeat(np.float32(10000.0) ** (-np.arange(0, ROT, 2, dtype=np.float32) / np.float32(ROT)), 2)
    keys = cache_len * groups
    kflat = kc.reshape(rows, keys, HEAD)
    vflat = vc.reshape(rows, keys, HEAD)
    vm = pl.BlockSpec(memory_space=pltpu.VMEM)
    hbm = pl.BlockSpec(memory_space=pl.ANY)
    bf, f32 = jnp.bfloat16, jnp.float32
    dma = pltpu.SemaphoreType.DMA
    hidden, m, ko, vo = pl.pallas_call(
        functools.partial(attn_kernel, rows=rows, blk=blk, heads=heads, groups=groups, qc=qc),
        name="attn",
        out_shape=(pltpu.VMEM((rows, hid), f32), pltpu.VMEM((rows, hid), bf),
                   jax.ShapeDtypeStruct(kflat.shape, bf), jax.ShapeDtypeStruct(vflat.shape, bf)),
        in_specs=[hbm] * 10,
        out_specs=(vm, vm, hbm, hbm),
        scratch_shapes=[
            pltpu.VMEM((rows, keys, HEAD), bf), pltpu.VMEM((rows, keys, HEAD), bf),
            pltpu.VMEM(wqkv.shape, bf), pltpu.VMEM(wproj.shape, bf),
            pltpu.SMEM((rows,), jnp.int32), pltpu.VMEM((1, HEAD), f32), pltpu.VMEM((rows, hid), bf),
            pltpu.VMEM(ga.shape, bf), pltpu.VMEM(bqkv.shape, bf), pltpu.VMEM(gm.shape, bf),
            pltpu.VMEM((rows, hid), bf), pltpu.VMEM((rows, HEAD), f32),
            pltpu.VMEM((rows * heads, HEAD), f32),
            pltpu.VMEM((rows * groups, HEAD), f32), pltpu.VMEM((rows * groups, HEAD), f32),
            pltpu.VMEM((blk // 2, 2 * heads, keys), f32), pltpu.VMEM((blk // 2, 2 * heads, keys), bf),
            pltpu.VMEM((rows * heads, HEAD), f32), pltpu.VMEM((rows, heads * HEAD), bf),
            dma((6,)), dma((wqkv.shape[1] // qc,)), dma(()),
            dma((nblk,)), dma((nblk,)), dma((nblk,)), dma((nblk,)),
        ],
        compiler_params=pltpu.CompilerParams(vmem_limit_bytes=60 * 1024 * 1024),
        cost_estimate=pl.CostEstimate(flops=2 * rows * hid * 4608 + 4 * rows * heads * keys * HEAD,
                                      bytes_accessed=86000000, transcendentals=rows * heads * keys),
    )(lens, jnp.asarray(freq), x, ga, wqkv, bqkv, wproj, gm, kflat, vflat)
    return hidden, m, ko.reshape(kc.shape), vo.reshape(vc.shape)


def mlp_kernel(hid_ref, m_ref, wi_hbm, wo_hbm, out_ref,
               wi, wt, wtr, wo, chip, gath, act, own_s, part_s, cps, crb, ps, rb, sb, t1, rr,
               wi_sem, wt_sem, wo_sem, peer_send, peer_recv, near_send, near_recv, rel_send, rel_recv,
               fw_send, fw_recv, cp_send, cp_recv, ps_send, ps_recv, rs_send, t1_recv, rr_recv,
               *, sizes, full, tail, fc, nc):
    rows, hid = m_ref.shape
    ncol = hid // nc
    first = [sum(sizes[:h]) for h in range(len(sizes))]
    bf, f32 = jnp.bfloat16, jnp.float32
    me = lax.axis_index('grp')
    core, xx, yy = me % 2, (me // 2) % 2, me // 4
    peer = me + 1 - 2 * core
    near = (me + 2 - 4 * xx, me + 4 - 8 * yy)

    def wi_copy(f, g):
        sl = pl.ds(f * fc, fc)
        return pltpu.make_async_copy(wi_hbm.at[g, sl], wi.at[g, sl], wi_sem.at[f, g])

    def wt_copy(g):
        return pltpu.make_async_copy(wi_hbm.at[g, pl.ds(full * fc, tail)], wt.at[g, pl.ds(0, tail)], wt_sem.at[g])

    wo_copy = pltpu.make_async_copy(wo_hbm, wo.at[pl.ds(0, full * fc + tail)], wo_sem)

    for f in range(full):
        for g in range(2):
            wi_copy(f, g).start()
    for g in range(2):
        wt_copy(g).start()
    wo_copy.start()

    def rcopy(src, dst, ss, rs, dev):
        return pltpu.make_async_remote_copy(src_ref=src, dst_ref=dst, send_sem=ss, recv_sem=rs,
                                            device_id={'grp': dev}, device_id_type=pl.DeviceIdType.MESH)

    def cols(c):
        return slice(c * nc, (c + 1) * nc)

    def g_at(h, slot, c=None):
        sl = pl.ds(6 * first[h] + slot * sizes[h], sizes[h])
        return gath.at[sl] if c is None else gath.at[sl, pl.ds(c * nc, nc)]

    to_peer = rcopy(m_ref, chip.at[pl.ds(rows, rows)], peer_send, peer_recv, peer)

    def to_near(h, d, c):
        return rcopy(m_ref.at[pl.ds(first[h], sizes[h]), pl.ds(c * nc, nc)], g_at(h, d, c),
                     near_send.at[h, d, c], near_recv.at[h, d, c], near[d])

    def relay(h, d):
        return rcopy(g_at(h, d, d), g_at(h, 2, d), rel_send.at[h, d], rel_recv.at[h, d], near[1 - d])

    def forward(h, s):
        return rcopy(g_at(h, s), g_at(h, 3 + s), fw_send.at[h, s], fw_recv.at[h, s], peer)

    def chip_send(c):
        sl = (slice(None), pl.ds(c * nc, nc))
        return rcopy(cps.at[sl], crb.at[sl], cp_send.at[c], cp_recv.at[c], peer)

    def pair_send(h, c):
        sl = (pl.ds(3 * first[h], 3 * sizes[h]), pl.ds(c * nc, nc))
        return rcopy(ps.at[sl], rb.at[sl], ps_send.at[h, c], ps_recv.at[h, c], peer)

    def sb_at(h, k):
        return slice(3 * first[h] + k * sizes[h], 3 * first[h] + (k + 1) * sizes[h])

    def rows_of(h):
        return slice(first[h], first[h] + sizes[h])

    def diag_send(h, c):
        return rcopy(sb.at[sb_at(h, 2), pl.ds(c * nc, nc)], t1.at[rows_of(h), pl.ds(c * nc, nc)],
                     rs_send.at[h, c, 2], t1_recv.at[h, c], near[c])

    def near_part(h, c, d):
        return rcopy(sb.at[sb_at(h, d), pl.ds(c * nc, nc)], rr.at[d, rows_of(h), pl.ds(c * nc, nc)],
                     rs_send.at[h, c, d], rr_recv.at[h, c, d], near[d])

    barrier = pltpu.get_barrier_semaphore()
    for dev in (peer,) + near:
        pl.semaphore_signal(barrier, inc=1, device_id={'grp': dev}, device_id_type=pl.DeviceIdType.MESH)
    pl.semaphore_wait(barrier, 3)

    def send_half(h, k):
        for d in range(2):
            to_near(h, d, k if d == 0 else 1 - k).start()

    def pass_on(h):
        for d in range(2):
            to_near(h, d, d).wait_recv()
            relay(h, d).start()

    def share(h):
        for d in range(2):
            to_near(h, d, 1 - d).wait_recv()
            forward(h, d).start()

    def share_diag(h):
        for d in range(2):
            relay(h, d).wait_recv()
        forward(h, 2).start()

    def all_here(h):
        for s in range(3):
            forward(h, s).wait_recv()

    to_peer.start()
    send_half(0, 0)
    send_half(0, 1)
    send_half(1, 0)
    for g in range(2):
        wt[g, tail:, :] = jnp.zeros((fc // 2 - tail, hid), bf)
    wo[full * fc + tail:, :] = jnp.zeros((fc // 2 - tail, hid), bf)
    chip[0:rows] = m_ref[...]

    def gated(gate, up):
        return (jax.nn.silu(gate) * up).astype(bf)

    for f in range(full + 1):
        n = fc if f < full else fc // 2
        sl = slice(f * fc, f * fc + n)
        for g in range(2):
            (wi_copy(f, g) if f < full else wt_copy(g)).wait()
            wtr[g, :, sl] = (wi[g, sl, :] if f < full else wt[g]).T
        if f == HOOK:
            pass_on(0)
            send_half(1, 1)
            share(0)

    def up_and_gate(g, n):
        for lo, hi in IN_CUTS:
            gate = jnp.dot(g, wtr[0, :, lo:hi], preferred_element_type=f32)
            up = jnp.dot(g, wtr[1, :, lo:hi], preferred_element_type=f32)
            act[0:n, lo:hi] = gated(gate, up)

    def own_rows():
        to_peer.wait_recv()
        up_and_gate(chip[...], 2 * rows)
        for c in range(ncol):
            part = jnp.dot(act[0:2 * rows, :], wo[:, cols(c)], preferred_element_type=f32)
            cps[:, cols(c)] = part[rows:].astype(bf)
            own_s[:, cols(c)] = part[:rows]
            chip_send(c).start()

    def in_proj(h):
        n = 6 * sizes[h]
        up_and_gate(gath[6 * first[h]:6 * first[h] + n, :], n)

    def out_proj(h):
        n = 3 * sizes[h]
        sl = slice(3 * first[h], 3 * first[h] + n)
        for c in range(ncol):
            part = jnp.dot(act[0:2 * n, :], wo[:, cols(c)], preferred_element_type=f32)
            ps[sl, cols(c)] = part[n:].astype(bf)
            part_s[sl, cols(c)] = part[:n]
            pair_send(h, c).start()

    def stage1(h):
        for c in range(ncol):
            pair_send(h, c).wait_recv()
            e, n = 1 - c, sizes[h]
            sl = slice(3 * first[h], 3 * first[h] + 3 * n)
            tot = part_s[sl, cols(c)] + rb[sl, cols(c)].astype(f32)
            part_s[sb_at(h, e), cols(c)] = tot[e * n:(e + 1) * n]
            sb[sb_at(h, 2), cols(c)] = tot[2 * n:].astype(bf)
            sb[sb_at(h, c), cols(c)] = tot[c * n:(c + 1) * n].astype(bf)
            diag_send(h, c).start()
            near_part(h, c, c).start()

    def stage2(h):
        for c in range(ncol):
            e = 1 - c
            diag_send(h, c).wait_recv()
            sb[sb_at(h, e), cols(c)] = (part_s[sb_at(h, e), cols(c)] + t1[rows_of(h), cols(c)].astype(f32)).astype(bf)
            near_part(h, c, e).start()

    def chip_sum(c):
        chip_send(c).wait_recv()
        own_s[:, cols(c)] = hid_ref[:, cols(c)] + own_s[:, cols(c)] + crb[:, cols(c)].astype(f32)

    def finish(h):
        for c in range(ncol):
            for d in range(2):
                near_part(h, c, d).wait_recv()
            tot = own_s[rows_of(h), cols(c)]
            for d in range(2):
                tot = tot + rr[d, rows_of(h), cols(c)].astype(f32)
            out_ref[rows_of(h), cols(c)] = tot.astype(bf)

    share_diag(0)
    pass_on(1)
    wo_copy.wait()
    all_here(0)
    in_proj(0)
    share(1)
    out_proj(0)
    share_diag(1)
    stage1(0)
    all_here(1)
    in_proj(1)
    out_proj(1)
    stage2(0)
    stage1(1)
    own_rows()
    stage2(1)
    for c in range(ncol):
        chip_sum(c)
    finish(0)
    finish(1)

    to_peer.wait_send()
    for c in range(ncol):
        chip_send(c).wait_send()
    for h in range(len(sizes)):
        for d in range(2):
            for c in range(2):
                to_near(h, d, c).wait_send()
            relay(h, d).wait_send()
        for s in range(3):
            forward(h, s).wait_send()
        for c in range(ncol):
            pair_send(h, c).wait_send()
            diag_send(h, c).wait_send()
            for d in range(2):
                near_part(h, c, d).wait_send()


HOOK = 5
SIZES = (32, 32)
IN_CUTS = ((0, 512), (512, 1024), (1024, 1408))


def mlp(hidden, m, w_in, w_out):
    rows, hid = m.shape
    ffn = w_out.shape[0]
    fc, nc = 256, hid // 2
    sizes = SIZES
    chunks = len(sizes)
    full, tail = ffn // fc, ffn % fc
    width = full * fc + fc // 2
    ncol = hid // nc
    vm = pl.BlockSpec(memory_space=pltpu.VMEM)
    hbm = pl.BlockSpec(memory_space=pl.ANY)
    bf, f32 = jnp.bfloat16, jnp.float32
    dma = pltpu.SemaphoreType.DMA
    return pl.pallas_call(
        functools.partial(mlp_kernel, sizes=sizes, full=full, tail=tail, fc=fc, nc=nc),
        name="mlp",
        out_shape=pltpu.VMEM((rows, hid), bf),
        in_specs=[vm, vm, hbm, hbm],
        out_specs=vm,
        scratch_shapes=[
            pltpu.VMEM((2, full * fc, hid), bf), pltpu.VMEM((2, fc // 2, hid), bf), pltpu.VMEM((2, hid, width), bf),
            pltpu.VMEM((width, hid), bf),
            pltpu.VMEM((2 * rows, hid), bf), pltpu.VMEM((6 * rows, hid), bf),
            pltpu.VMEM((max(2 * rows, 6 * max(sizes)), width), bf),
            pltpu.VMEM((rows, hid), f32), pltpu.VMEM((3 * rows, hid), f32),
            pltpu.VMEM((rows, hid), bf), pltpu.VMEM((rows, hid), bf),
            pltpu.VMEM((3 * rows, hid), bf), pltpu.VMEM((3 * rows, hid), bf),
            pltpu.VMEM((3 * rows, hid), bf), pltpu.VMEM((rows, hid), bf), pltpu.VMEM((2, rows, hid), bf),
            dma((full, 2)), dma((2,)), dma(()),
            dma(()), dma(()), dma((chunks, 2, 2)), dma((chunks, 2, 2)), dma((chunks, 2)), dma((chunks, 2)),
            dma((chunks, 3)), dma((chunks, 3)), dma((ncol,)), dma((ncol,)), dma((chunks, ncol)), dma((chunks, ncol)),
            dma((chunks, ncol, 3)), dma((chunks, ncol)), dma((chunks, ncol, 2)),
        ],
        compiler_params=pltpu.CompilerParams(collective_id=0, has_side_effects=True, vmem_limit_bytes=46 << 20),
        cost_estimate=pl.CostEstimate(flops=2 * 8 * rows * hid * ffn * 3, bytes_accessed=17000000, transcendentals=8 * rows * ffn),
    )(pltpu.with_memory_space_constraint(hidden, pltpu.VMEM), pltpu.with_memory_space_constraint(m, pltpu.VMEM),
      pltpu.with_memory_space_constraint(w_in, pltpu.HBM), pltpu.with_memory_space_constraint(w_out, pltpu.HBM))


def solution(mesh):
    row_spec = P(('rep', 'grp'))
    repl_spec = P()

    def local_layer(x_in, seq_len, k_cache, v_cache, gamma_attn, w_qkv, b_qkv, w_proj, gamma_mlp, w_in, w_out):
        hidden, mlp_in, k_out, v_out = attention(x_in, seq_len, k_cache, v_cache, gamma_attn, w_qkv, b_qkv, w_proj, gamma_mlp)
        layer_out = mlp(hidden, mlp_in, w_in, w_out)
        return layer_out, k_out, v_out

    return jax.shard_map(local_layer, mesh=mesh,
                         in_specs=(row_spec, row_spec, row_spec, row_spec, repl_spec, repl_spec, repl_spec,
                                   repl_spec, repl_spec, P(None, 'grp', None), P('grp', None)),
                         out_specs=(row_spec, row_spec, row_spec), check_vma=False)
```
